32 devices in a mesh: seq: 8 (over y, x, core), head: 4 (over z).
Axes of the slice: x: 2, y: 2, z: 4, core: 2. Of those that a mesh axis runs over, the one named last changes fastest.
Arguments:
- queries: bfloat16 [2048, 4096], P('seq', 'head'), may hold values from -7.1875 to 7.1875
- keys: bfloat16 [2048, 1024], P(('seq', 'head')), may hold values from -7.1875 to 7.1875
- values: bfloat16 [2048, 1024], P(('seq', 'head')), may hold values from -6 to 6
- outputs: bfloat16 [2048, 4096], P('seq', 'head'), may hold values from -1.1953125 to 1.1953125
- out_grad: bfloat16 [2048, 4096], P('seq', 'head'), may hold values from -6 to 6
- log_norm: float32 [32, 2048], P('head', 'seq'), as said below
- block_order: int32 [16], replicated, may hold values from 0 to 15, as said below
Outputs:
- query_grad: bfloat16 [2048, 4096], P('seq', 'head')
- key_gradient_rows: bfloat16 [2048, 1024], P(('seq', 'head'))
- value_gradient_rows: bfloat16 [2048, 1024], P(('seq', 'head'))
The draws below stay inside these ranges and needn't reach their ends.
Inputs may be any that keep to these rules, and one draw needn't show every extreme that they name: `block_order`: A permutation of 0 to 15. log_norm[h, i] lies within 0.6 of one plus the natural logarithm of 1 + pos[i].
All inputs are finite; a program needn't handle non-finite values.
Results may differ from the reference program's by a relative error of at most 0.014.
Values may be sent and summed in bfloat16 or wider, within the bound.
No kernel may reach another device: no remote copies, remote signals or barrier semaphores. Data moves between devices by JAX's collectives and lax.ppermute only.
A program may use at most 192 MiB of HBM per device.

```python
import jax
import jax.numpy as jnp
from jax import lax

QUERY_HEADS = 32
KEY_VALUE_HEADS = 8
HEAD_SIZE = 128
TOK_DEV = 256
SEQUENCE_TOKENS = 2048
N_SEQ = 8


def order_helper(key):
    return jax.random.permutation(jax.random.fold_in(key, 7), 2 * N_SEQ).astype(jnp.int32)


def draw_block_order(key, part):
    return order_helper(key)


def draw_log_norm(key, part):
    order = order_helper(key)
    half = TOK_DEV // 2
    rows = jnp.arange(SEQUENCE_TOKENS, dtype=jnp.int32)
    pos = (order[rows // half] * half + rows % half).astype(jnp.float32)
    base = jnp.log(1.0 + pos)[None, :] + 1.0
    noise = jax.random.uniform(jax.random.fold_in(key, 11), (QUERY_HEADS, SEQUENCE_TOKENS), jnp.float32, -0.3, 0.3)
    return (base + noise).astype(jnp.float32)


def block_levels(rng, shape, shards, smallest, top_value):
    level = 1.0
    for position, parts in shards:
        heights = jax.random.uniform(jax.random.fold_in(jax.random.fold_in(rng, 6), position), (parts,), jnp.float32, smallest / len(shards), top_value / len(shards))
        level = level * jnp.repeat(jnp.exp(heights), shape[position] // parts).reshape((-1,) + (1,) * (len(shape) - 1 - position))
    return level


def gaussian(key, extent, width, most, pieces=(), kind=jnp.bfloat16):
    entries = jax.random.normal(key, extent, jnp.float32) * width
    if len(pieces) > 0:
        entries = block_levels(key, extent, pieces, -0.22, 0.18) * entries
    return jnp.clip(entries, min=-most, max=most).astype(kind)


def setup_inputs(seed: int = 0) -> dict:
    streams_of = jax.random.split(jax.random.key(seed), 8)
    queries = gaussian(streams_of[0], (SEQUENCE_TOKENS, QUERY_HEADS * HEAD_SIZE), 1.2, 7.1875, ((0, 8), (1, 4)))
    keys = gaussian(streams_of[1], (SEQUENCE_TOKENS, KEY_VALUE_HEADS * HEAD_SIZE), 1.2, 7.1875, ((0, 32),))
    values = gaussian(streams_of[2], (SEQUENCE_TOKENS, KEY_VALUE_HEADS * HEAD_SIZE), 1.0, 6.0, ((0, 32),))
    outputs = gaussian(streams_of[3], (SEQUENCE_TOKENS, QUERY_HEADS * HEAD_SIZE), 0.2, 1.1953125, ((0, 8), (1, 4)))
    out_grad = gaussian(streams_of[4], (SEQUENCE_TOKENS, QUERY_HEADS * HEAD_SIZE), 1.0, 6.0, ((0, 8), (1, 4)))
    log_norm = draw_log_norm(jax.random.fold_in(streams_of[7], 71), 0)
    block_order = draw_block_order(jax.random.fold_in(streams_of[7], 71), 0)
    return {"queries": queries, "keys": keys, "values": values, "outputs": outputs, "out_grad": out_grad, "log_norm": log_norm, "block_order": block_order}


def token_positions(block_order):
    half = TOK_DEV // 2
    rows = jnp.arange(SEQUENCE_TOKENS, dtype=jnp.int32)
    return (block_order[rows // half] * half + rows % half).astype(jnp.int32)


def reference(queries, keys, values, outputs, out_grad, log_norm, block_order):
    scale = HEAD_SIZE ** -0.5
    group_ratio = QUERY_HEADS // KEY_VALUE_HEADS
    pos = token_positions(block_order)
    delta = jnp.sum((out_grad.astype(jnp.float32) * outputs.astype(jnp.float32)).reshape(SEQUENCE_TOKENS, QUERY_HEADS, HEAD_SIZE), -1)
    qblock = 512 if SEQUENCE_TOKENS % 512 == 0 else SEQUENCE_TOKENS
    nblocks = SEQUENCE_TOKENS // qblock

    def queries_per_group(g):
        kg = lax.dynamic_slice_in_dim(keys, g * HEAD_SIZE, HEAD_SIZE, 1).astype(jnp.float32)
        vg = lax.dynamic_slice_in_dim(values, g * HEAD_SIZE, HEAD_SIZE, 1).astype(jnp.float32)
        qg = lax.dynamic_slice_in_dim(queries, g * group_ratio * HEAD_SIZE, group_ratio * HEAD_SIZE, 1).reshape(SEQUENCE_TOKENS, group_ratio, HEAD_SIZE)
        dg = lax.dynamic_slice_in_dim(out_grad, g * group_ratio * HEAD_SIZE, group_ratio * HEAD_SIZE, 1).reshape(SEQUENCE_TOKENS, group_ratio, HEAD_SIZE)
        lg = lax.dynamic_slice_in_dim(log_norm, g * group_ratio, group_ratio, 0)
        eg = lax.dynamic_slice_in_dim(delta, g * group_ratio, group_ratio, 1)

        def step(carry, b):
            keys_gradient, values_gradient = carry
            start = (b * qblock).astype(jnp.int32)
            qb = lax.dynamic_slice_in_dim(qg, start, qblock, 0).astype(jnp.float32)
            db = lax.dynamic_slice_in_dim(dg, start, qblock, 0).astype(jnp.float32)
            lb = lax.dynamic_slice_in_dim(lg, start, qblock, 1)
            eb = lax.dynamic_slice_in_dim(eg, start, qblock, 0)
            qpos = lax.dynamic_slice_in_dim(pos, start, qblock, 0)
            scores = jnp.einsum("trd,nd->rtn", qb, kg) * scale
            visible = pos[None, :] <= qpos[:, None]
            prob = jnp.where(visible[None], jnp.exp(scores - lb[:, :, None]), 0.0)
            dprob = jnp.einsum("trd,nd->rtn", db, vg)
            dscore = prob * (dprob - eb.T[:, :, None])
            prob_low = prob.astype(jnp.bfloat16).astype(jnp.float32)
            dscore_low = dscore.astype(jnp.bfloat16).astype(jnp.float32)
            values_gradient = values_gradient + jnp.einsum("rtn,trd->nd", prob_low, db)
            keys_gradient = keys_gradient + scale * jnp.einsum("rtn,trd->nd", dscore_low, qb)
            queries_gradient = scale * jnp.einsum("rtn,nd->trd", dscore_low, kg)
            return (keys_gradient, values_gradient), queries_gradient.astype(jnp.bfloat16)

        zeros = jnp.zeros((SEQUENCE_TOKENS, HEAD_SIZE), jnp.float32)
        (keys_gradient, values_gradient), queries_gradient = lax.scan(step, (zeros, zeros), jnp.arange(nblocks, dtype=jnp.int32))
        return queries_gradient.reshape(SEQUENCE_TOKENS, group_ratio * HEAD_SIZE), keys_gradient.astype(jnp.bfloat16), values_gradient.astype(jnp.bfloat16)

    queries_gradient, keys_gradient, values_gradient = lax.map(queries_per_group, jnp.arange(KEY_VALUE_HEADS, dtype=jnp.int32))
    query_grad = jnp.transpose(queries_gradient, (1, 0, 2)).reshape(SEQUENCE_TOKENS, QUERY_HEADS * HEAD_SIZE)
    key_gradient_rows = jnp.transpose(keys_gradient, (1, 0, 2)).reshape(SEQUENCE_TOKENS, KEY_VALUE_HEADS * HEAD_SIZE)
    value_gradient_rows = jnp.transpose(values_gradient, (1, 0, 2)).reshape(SEQUENCE_TOKENS, KEY_VALUE_HEADS * HEAD_SIZE)
    return (query_grad, key_gradient_rows, value_gradient_rows)
```

```python
import functools

import jax
import jax.numpy as jnp
from jax import lax
from jax.experimental import pallas as pl
from jax.experimental.pallas import tpu as pltpu
from jax.sharding import Mesh
from jax.sharding import PartitionSpec as P

QUERY_HEADS = 32
KEY_VALUE_HEADS = 8
HEAD_SIZE = 128
LOG2E = 1.4426950408889634
SCALE = HEAD_SIZE ** (-0.5)
RATIO = QUERY_HEADS // KEY_VALUE_HEADS


VMEM = pl.BlockSpec(memory_space=pltpu.VMEM)
SMEM = pl.BlockSpec(memory_space=pltpu.SMEM)


def sds(shape, dtype):
    return jax.ShapeDtypeStruct(shape, dtype)


def cost(flops, size):
    return pl.CostEstimate(flops=int(flops), bytes_accessed=int(size), transcendentals=0)


def pack_kernel(meta, keys, values, *outs):
    core, z = meta[0], meta[1]
    for m, out in enumerate(outs):
        group = jnp.bitwise_xor(z, m)
        for j in range(2):
            col = (2 * group + jnp.bitwise_xor(core, j)) * HEAD_SIZE
            col = pl.multiple_of(col, HEAD_SIZE)
            out[j, 0] = keys[:, pl.ds(col, HEAD_SIZE)]
            out[j, 1] = values[:, pl.ds(col, HEAD_SIZE)]


def pack(meta, keys, values, n_heads):
    piece = keys.shape[0]
    shape = (2, 2, piece, HEAD_SIZE)
    return pl.pallas_call(
        pack_kernel,
        in_specs=[SMEM, VMEM, VMEM],
        out_specs=[VMEM] * n_heads,
        out_shape=[sds(shape, keys.dtype)] * n_heads,
        cost_estimate=cost(1000, 4 * keys.size * 2),
        name="pack_kv",
    )(meta, keys, values)


def prepare_kernel(meta, q, do, o, lse, q_send, do_send, stats_own, stats_send):
    core = meta[0]
    heads = lse.shape[0]
    cols = q_send.shape[1]
    rows = []
    for h in range(heads):
        a = do[:, h * HEAD_SIZE : (h + 1) * HEAD_SIZE].astype(jnp.float32)
        b = o[:, h * HEAD_SIZE : (h + 1) * HEAD_SIZE].astype(jnp.float32)
        rows.append(jnp.sum((a * b).T, axis=0, keepdims=True))
    scaled = lse[...] * LOG2E
    low = jnp.concatenate([scaled[:RATIO]] + rows[:RATIO], 0)
    high = jnp.concatenate([scaled[RATIO:]] + rows[RATIO:], 0)
    stats_own[...] = jnp.where(core == 0, low, high)
    stats_send[...] = jnp.where(core == 0, high, low)

    @pl.when(core == 0)
    def _():
        q_send[...] = q[:, cols:]
        do_send[...] = do[:, cols:]

    @pl.when(core != 0)
    def _():
        q_send[...] = q[:, :cols]
        do_send[...] = do[:, :cols]


def prepare(meta, q, do, o, lse):
    tok, cols = q.shape
    part = sds((tok, cols // 2), q.dtype)
    stats = sds((2 * RATIO, tok), jnp.float32)
    return pl.pallas_call(
        prepare_kernel,
        in_specs=[SMEM, VMEM, VMEM, VMEM, VMEM],
        out_specs=[VMEM] * 4,
        out_shape=[part, part, stats, stats],
        cost_estimate=cost(1000, 8 * q.size),
        name="prepare_q",
    )(meta, q, do, o, lse)


def chunk_kernel(first, last, tile, meta, q0, q1, do0, do1, stats0, stats1, kv, *rest):
    if first:
        acc_in = None
    else:
        acc_in, rest = rest[0], rest[1:]
    if last:
        dq0, dq1, dkv, dk_acc, dv_acc, acc = rest
    else:
        acc, dkv, dk_acc, dv_acc = rest
    n_rows = kv.shape[1]
    tok = q0.shape[0]
    half = tok // 2
    q_blocks = 4
    piece_xor = meta[0]
    dk_acc[...] = jnp.zeros_like(dk_acc)
    dv_acc[...] = jnp.zeros_like(dv_acc)
    width = RATIO * half
    if first:
        acc[...] = jnp.zeros_like(acc)
    elif last:
        acc[...] = acc_in[...]
    for b in range(q_blocks):
        q_ref = q0 if b < 2 else q1
        do_ref = do0 if b < 2 else do1
        stats = stats0 if b < 2 else stats1
        r0 = (b % 2) * half
        q_id = meta[1 + b]
        for t in range(n_rows // tile):
            per = tile // half
            ids = [meta[1 + q_blocks + t * per + i] for i in range(per)]
            lowest = functools.reduce(jnp.minimum, ids)

            @pl.when(lowest <= q_id)
            def _(b=b, t=t, ids=ids, q_ref=q_ref, do_ref=do_ref, stats=stats, r0=r0, q_id=q_id):
                cols = [slice(h * HEAD_SIZE, (h + 1) * HEAD_SIZE) for h in range(RATIO)]
                qs = jnp.concatenate([q_ref[r0 : r0 + half, c] for c in cols], 0)
                dos = jnp.concatenate([do_ref[r0 : r0 + half, c] for c in cols], 0)
                k = kv[0, t * tile : (t + 1) * tile, :]
                v = kv[1, t * tile : (t + 1) * tile, :]
                nt = (((1,), (1,)), ((), ()))
                s = lax.dot_general(k, qs, nt, preferred_element_type=jnp.float32)
                dp = lax.dot_general(v, dos, nt, preferred_element_type=jnp.float32)
                row = lax.broadcasted_iota(jnp.int32, (half, half), 0)
                lane = lax.broadcasted_iota(jnp.int32, (half, half), 1)
                offset = jnp.bitwise_xor(row, piece_xor) - lane
                ahead = jnp.concatenate([offset + (i - q_id) * half for i in ids], 0)
                visible = ahead <= 0
                probs, scores = [], []
                for h in range(RATIO):
                    c = slice(h * half, (h + 1) * half)
                    lse = stats[h : h + 1, r0 : r0 + half]
                    delta = stats[RATIO + h : RATIO + h + 1, r0 : r0 + half]
                    p = jnp.where(visible, jnp.exp2(s[:, c] * (SCALE * LOG2E) - lse), 0.0)
                    probs.append(p.astype(jnp.bfloat16))
                    scores.append((p * (dp[:, c] - delta)).astype(jnp.bfloat16))
                prob = jnp.concatenate(probs, 1)
                score = jnp.concatenate(scores, 1)
                rows = slice(t * tile, (t + 1) * tile)
                dv_acc[rows, :] += jnp.dot(prob, dos, preferred_element_type=jnp.float32)
                dk_acc[rows, :] += jnp.dot(score, qs, preferred_element_type=jnp.float32)
                acc[:, b * width : (b + 1) * width] += jnp.dot(
                    k.T, score, preferred_element_type=jnp.float32
                )

    dkv[0] = (dk_acc[...] * SCALE).astype(dkv.dtype)
    dkv[1] = dv_acc[...].astype(dkv.dtype)
    if last:
        for b in range(q_blocks):
            out = dq0 if b < 2 else dq1
            r0 = (b % 2) * half
            for h in range(RATIO):
                c = b * width + h * half
                block = (acc[:, c : c + half] * SCALE).T
                out[r0 : r0 + half, h * HEAD_SIZE : (h + 1) * HEAD_SIZE] = block.astype(out.dtype)


def chunk(core, meta, q, q1, do, do1, stats0, stats1, kv, acc, last, out_dtype):
    tok, cols = q1.shape
    n_rows = kv.shape[1]
    first = acc is None
    acc_shape = sds((HEAD_SIZE, 4 * RATIO * (tok // 2)), jnp.float32)
    tile = min(n_rows, 256)
    own = lambda: pl.BlockSpec((tok, cols), lambda i, m, c: (0, c[0]))
    full = lambda s: pl.BlockSpec(s, lambda i, m, c: (0,) * len(s))
    in_specs = [own(), full((tok, cols)), own(), full((tok, cols)), full(stats0.shape), full(stats1.shape), full(kv.shape)]
    args = [q, q1, do, do1, stats0, stats1, kv]
    if not first:
        in_specs.append(full(acc_shape.shape))
        args.append(acc)
    dkv_shape = sds(kv.shape, out_dtype)
    scratch = [pltpu.VMEM((n_rows, HEAD_SIZE), jnp.float32)] * 2
    if last:
        outs = [sds((tok, cols), q.dtype)] * 2 + [dkv_shape]
        scratch = scratch + [pltpu.VMEM(acc_shape.shape, jnp.float32)]
        aliases = {}
    else:
        outs = [acc_shape, dkv_shape]
        aliases = {}

    def body(m, c, *refs):
        if not first and not last:
            refs = list(refs)
            ins, acc_in, acc_out = refs[:7], refs[7], refs[8]
            acc_out[...] = acc_in[...]
            chunk_kernel(False, False, tile, m, *ins, None, *refs[8:])
        else:
            chunk_kernel(first, last, tile, m, *refs)

    flops = 5 * 2 * n_rows * 2 * tok * cols
    return pl.pallas_call(
        body,
        grid_spec=pltpu.PrefetchScalarGridSpec(
            num_scalar_prefetch=2,
            grid=(1,),
            in_specs=in_specs,
            out_specs=[full(s.shape) for s in outs],
            scratch_shapes=scratch,
        ),
        out_shape=outs,
        input_output_aliases=aliases,
        cost_estimate=cost(flops, 4 * q.size * 2),
        name="chunk",
    )(meta, core, *args)


def collect_kernel(own, *rest):
    n = len(rest) // 2
    received, outs = rest[:-1], rest[-1]
    total = own[...]
    for r in received:
        total = total + r[...].astype(jnp.float32)
    outs[...] = total


def collect(own, received, n_heads):
    rows = own.shape[1]
    piece = rows // (2 * n_heads)

    def body(own_ref, *refs):
        received, outs = refs[: len(refs) - n_heads], refs[len(refs) - n_heads :]
        for m, out in enumerate(outs):
            for j in range(2):
                r0 = (j * n_heads + m) * piece
                for a in range(2):
                    total = own_ref[a, r0 : r0 + piece, :]
                    for r in received:
                        total = total + r[a, r0 : r0 + piece, :].astype(jnp.float32)
                    out[j, a] = total.astype(out.dtype)

    shape = sds((2, 2, piece, HEAD_SIZE), jnp.bfloat16)
    return pl.pallas_call(
        body,
        in_specs=[VMEM] * (1 + len(received)),
        out_specs=[VMEM] * n_heads,
        out_shape=[shape] * n_heads,
        cost_estimate=cost(1000, 8 * own.size),
        name="collect",
    )(own, *received)


def unpack_kernel(n, meta, *refs):
    core, z = meta[0], meta[1]
    mine, theirs, dk, dv = refs[:n], refs[n : 2 * n], refs[2 * n], refs[2 * n + 1]
    for m in range(n):
        group = jnp.bitwise_xor(z, m)
        for j, (a, b) in enumerate(((mine[m][0, 0], mine[m][0, 1]), (theirs[m][0], theirs[m][1]))):
            col = (2 * group + jnp.bitwise_xor(core, j)) * HEAD_SIZE
            col = pl.multiple_of(col, HEAD_SIZE)
            dk[:, pl.ds(col, HEAD_SIZE)] = a
            dv[:, pl.ds(col, HEAD_SIZE)] = b


def unpack(meta, mine, theirs):
    n = len(mine)
    piece = mine[0].shape[2]
    out = sds((piece, KEY_VALUE_HEADS * HEAD_SIZE), jnp.bfloat16)
    return pl.pallas_call(
        functools.partial(unpack_kernel, n),
        in_specs=[SMEM] + [VMEM] * (2 * n),
        out_specs=[VMEM] * 2,
        out_shape=[out] * 2,
        cost_estimate=cost(1000, 8 * piece * 1024),
        name="unpack_kv",
    )(meta, *mine, *theirs)


def exchange(x, axis, size, m):
    return lax.ppermute(x, axis, [(i, i ^ m) for i in range(size)])


def local(n_chips, n_heads, queries, keys, values, outputs, out_grad, log_norm, block_order):
    c, core, z = lax.axis_index("chip"), lax.axis_index("core"), lax.axis_index("head")
    tok, cols = queries.shape
    half = tok // 2
    piece = keys.shape[0]
    per_block = half // piece
    where = jnp.stack([core, z])

    zs = pack(where, keys, values, n_heads)
    order = sorted(range(1, n_heads), key=lambda m: -(m ^ 1))
    zr = {0: zs[0]}
    for m in order:
        zr[m] = exchange(zs[m], "head", n_heads, m)
    q_send, do_send, stats0, stats_send = prepare(where, queries, out_grad, outputs, log_norm)
    q1 = exchange(q_send, "core", 2, 1)
    do1 = exchange(do_send, "core", 2, 1)
    stats1 = exchange(stats_send, "core", 2, 1)
    cr = [exchange(zr[m][1], "core", 2, 1) for m in range(n_heads)]
    kv = jnp.concatenate([zr[m][0] for m in range(n_heads)] + cr, 1)

    table = block_order.reshape(n_chips, 2, 2)
    table = jnp.where(core == 0, table, table[:, ::-1])
    slot_xor = z // per_block
    kblocks = table[:, :, :]
    if n_heads // per_block > 1:
        kblocks = jnp.where(slot_xor % 2 == 0, table, table[:, :, ::-1])
    q_ids = lax.dynamic_slice_in_dim(table, c, 1, 0).reshape(4)
    piece_xor = (piece * (z % per_block)).astype(jnp.int32)

    kvs = [kv] + [exchange(kv, "chip", n_chips, m) for m in range(1, n_chips)]
    acc = None
    own = None
    received = []
    for m in range(n_chips):
        k_ids = lax.dynamic_slice_in_dim(kblocks, jnp.bitwise_xor(c, m), 1, 0).reshape(4)
        meta = jnp.concatenate([piece_xor[None], q_ids, k_ids]).astype(jnp.int32)
        last = m == n_chips - 1
        out = chunk(
            core[None], meta, queries, q1, out_grad, do1, stats0, stats1, kvs[m], acc, last,
            jnp.float32 if m == 0 else jnp.bfloat16,
        )
        if last:
            dq0, dq_send, dkv = out
        else:
            acc, dkv = out
        if m == 0:
            own = dkv
        else:
            received.append(exchange(dkv, "chip", n_chips, m))
    dq1 = exchange(dq_send, "core", 2, 1)
    slots = collect(own, received, n_heads)
    back = {0: slots[0]}
    for m in order:
        back[m] = exchange(slots[m], "head", n_heads, m)
    theirs = [exchange(back[m][1], "core", 2, 1) for m in range(n_heads)]
    dk, dv = unpack(where, [back[m] for m in range(n_heads)], theirs)
    dq = jnp.where(core == 0, jnp.concatenate([dq0, dq1], 1), jnp.concatenate([dq1, dq0], 1))
    return dq, dk, dv


def solution(mesh):
    n_seq, n_heads = mesh.shape["seq"], mesh.shape["head"]
    n_chips = n_seq // 2
    fine = Mesh(mesh.devices.reshape(n_chips, 2, n_heads), ("chip", "core", "head"))
    seq = ("chip", "core")
    rows, tokens = P(seq, "head"), P(("chip", "core", "head"), None)
    in_specs = (rows, tokens, tokens, rows, rows, P("head", seq), P())
    out_specs = (rows, tokens, tokens)
    return jax.shard_map(
        functools.partial(local, n_chips, n_heads),
        mesh=fine,
        in_specs=in_specs,
        out_specs=out_specs,
        check_vma=False,
    )
```

```python
import functools

import jax
import jax.numpy as jnp
from jax import lax
from jax.experimental import pallas as pl
from jax.experimental.pallas import tpu as pltpu
from jax.sharding import Mesh
from jax.sharding import PartitionSpec as P


QUERY_HEADS = 32
KEY_VALUE_HEADS = 8
HEAD_SIZE = 128
LOG2E = 1.4426950408889634
SCALE = HEAD_SIZE ** (-0.5)
RATIO = QUERY_HEADS // KEY_VALUE_HEADS


VMEM = pl.BlockSpec(memory_space=pltpu.VMEM)
SMEM = pl.BlockSpec(memory_space=pltpu.SMEM)


def sds(shape, dtype):
    return jax.ShapeDtypeStruct(shape, dtype)


def cost(flops, size):
    return pl.CostEstimate(flops=int(flops), bytes_accessed=int(size), transcendentals=0)


def near(x):
    return pltpu.with_memory_space_constraint(x, pltpu.VMEM)


def params(mib=16):
    return pltpu.CompilerParams(vmem_limit_bytes=mib << 20)


def pack_kernel(where, keys, values, *outs):
    core, z = where[1], where[2]
    for m, out in enumerate(outs):
        group = jnp.bitwise_xor(z, m)
        for j in range(2):
            col = (2 * group + jnp.bitwise_xor(core, j)) * HEAD_SIZE
            col = pl.multiple_of(col, HEAD_SIZE)
            out[j, 0] = keys[:, pl.ds(col, HEAD_SIZE)]
            out[j, 1] = values[:, pl.ds(col, HEAD_SIZE)]


def pack(where, keys, values, n_heads):
    shape = (2, 2, keys.shape[0], HEAD_SIZE)
    return pl.pallas_call(
        pack_kernel,
        in_specs=[SMEM, VMEM, VMEM],
        out_specs=[VMEM] * n_heads,
        out_shape=[pltpu.VMEM(shape, keys.dtype)] * n_heads,
        compiler_params=params(8),
        cost_estimate=cost(1e6, 4 * keys.size * 2),
        name="pack_kv",
    )(where, keys, values)


def prepare_kernel(where, q, do, o, lse, q_own, do_own, stats_own, q_send, do_send, stats_send):
    core = where[1]
    half = q.shape[0] // 2
    rows = []
    for h in range(lse.shape[0]):
        a = do[:, h * HEAD_SIZE : (h + 1) * HEAD_SIZE].astype(jnp.float32)
        b = o[:, h * HEAD_SIZE : (h + 1) * HEAD_SIZE].astype(jnp.float32)
        rows.append(jnp.sum((a * b).T, axis=0, keepdims=True))
    scaled = lse[...] * LOG2E
    low = jnp.concatenate([scaled[:RATIO]] + rows[:RATIO], 0)
    high = jnp.concatenate([scaled[RATIO:]] + rows[RATIO:], 0)
    stats_own[...] = jnp.where(core == 0, low, high)
    stats_send[...] = jnp.where(core == 0, high, low)

    def copy(first, q_out, do_out):
        for b in range(2):
            for h in range(RATIO):
                src = (slice(b * half, (b + 1) * half), slice((first + h) * HEAD_SIZE, (first + h + 1) * HEAD_SIZE))
                dst = slice((b * RATIO + h) * half, (b * RATIO + h + 1) * half)
                q_out[dst, :] = q[src]
                do_out[dst, :] = do[src]

    @pl.when(core == 0)
    def _():
        copy(0, q_own, do_own)
        copy(RATIO, q_send, do_send)

    @pl.when(core != 0)
    def _():
        copy(RATIO, q_own, do_own)
        copy(0, q_send, do_send)


def prepare(where, q, do, o, lse):
    tok = q.shape[0]
    part = pltpu.VMEM((tok * RATIO, HEAD_SIZE), q.dtype)
    stats = pltpu.VMEM((2 * RATIO, tok), jnp.float32)
    return pl.pallas_call(
        prepare_kernel,
        in_specs=[SMEM, VMEM, VMEM, VMEM, VMEM],
        out_specs=[VMEM] * 6,
        out_shape=[part, part, stats] * 2,
        compiler_params=params(16),
        cost_estimate=cost(1e7, 8 * q.size),
        name="prepare_q",
    )(where, q, do, o, lse)


def assemble_kernel(n_slots, *refs):
    out = refs[-1]
    for s in range(n_slots):
        out[s] = refs[s][0]
        out[n_slots + s] = refs[n_slots + s][1]


def assemble(mine, theirs):
    n_slots = len(mine)
    shape = (2 * n_slots,) + mine[0].shape[1:]
    return pl.pallas_call(
        functools.partial(assemble_kernel, n_slots),
        in_specs=[VMEM] * (2 * n_slots),
        out_specs=VMEM,
        out_shape=pltpu.VMEM(shape, mine[0].dtype),
        compiler_params=params(8),
        cost_estimate=cost(1e6, 1e6),
        name="assemble",
    )(*[near(x) for x in mine], *[near(x) for x in theirs])


def chunk_kernel(m, slots, first, where, order, q0, do0, stats0, q1, do1, stats1, kv, *rest):
    acc, dkv = rest[-2:]
    c, core, z = where[0], where[1], where[2]
    n_slots = len(slots)
    piece = kv.shape[2]
    half = stats0.shape[1] // 2
    width = RATIO * half
    per_block = half // piece
    other = jnp.bitwise_xor(c, m)
    starts = []
    for j in range(2):
        for slot in slots:
            source = jnp.bitwise_xor(z, slot)
            block = order[(other * 2 + jnp.bitwise_xor(core, j)) * 2 + source // per_block]
            starts.append(block * half + (source % per_block) * piece)
    row = lax.broadcasted_iota(jnp.int32, (piece, half), 0)
    lane = lax.broadcasted_iota(jnp.int32, (piece, half), 1)
    k = jnp.concatenate([kv[p, 0] for p in range(2 * n_slots)], 0)
    v = jnp.concatenate([kv[p, 1] for p in range(2 * n_slots)], 0)
    kt = k.T
    nt = (((1,), (1,)), ((), ()))
    dk = dv = None
    for b in range(4):
        q_ref, do_ref, stats = (q0, do0, stats0) if b < 2 else (q1, do1, stats1)
        i = b % 2
        lo = order[(c * 2 + jnp.bitwise_xor(core, b // 2)) * 2 + i] * half
        qs = q_ref[i * width : (i + 1) * width, :]
        dos = do_ref[i * width : (i + 1) * width, :]
        s = lax.dot_general(k, qs, nt, preferred_element_type=jnp.float32)
        dp = lax.dot_general(v, dos, nt, preferred_element_type=jnp.float32)
        visible = jnp.concatenate([row - lane for _ in starts], 0) <= jnp.concatenate(
            [jnp.full((piece, half), lo - start, jnp.int32) for start in starts], 0
        )
        probs, scores = [], []
        for h in range(RATIO):
            cols = slice(h * half, (h + 1) * half)
            lse = stats[h : h + 1, i * half : (i + 1) * half]
            delta = stats[RATIO + h : RATIO + h + 1, i * half : (i + 1) * half]
            p = jnp.where(visible, jnp.exp2(s[:, cols] * (SCALE * LOG2E) - lse), 0.0)
            probs.append(p.astype(jnp.bfloat16))
            scores.append((p * (dp[:, cols] - delta)).astype(jnp.bfloat16))
        prob = jnp.concatenate(probs, 1)
        score = jnp.concatenate(scores, 1)
        dv_b = jnp.dot(prob, dos, preferred_element_type=jnp.float32)
        dk_b = jnp.dot(score, qs, preferred_element_type=jnp.float32)
        dv = dv_b if dv is None else dv + dv_b
        dk = dk_b if dk is None else dk + dk_b
        dq = jnp.dot(kt, score, preferred_element_type=jnp.float32)
        if first:
            acc[:, b * width : (b + 1) * width] = dq
        else:
            acc[:, b * width : (b + 1) * width] = rest[0][:, b * width : (b + 1) * width] + dq
    for p in range(2 * n_slots):
        dkv[p, 0] = (dk[p * piece : (p + 1) * piece] * SCALE).astype(dkv.dtype)
        dkv[p, 1] = dv[p * piece : (p + 1) * piece].astype(dkv.dtype)


def chunk(m, slots, where, order, q_side, kv, acc, out_dtype):
    first = acc is None
    width = q_side[0].shape[0] * 2
    acc_out = pltpu.VMEM((HEAD_SIZE, width), jnp.float32)
    args = [near(x) for x in q_side] + [near(kv)] + ([] if first else [near(acc)])
    rows = kv.shape[0] * kv.shape[2]
    return pl.pallas_call(
        functools.partial(chunk_kernel, m, slots, first),
        in_specs=[SMEM, SMEM] + [VMEM] * len(args),
        out_specs=[VMEM] * 2,
        out_shape=[acc_out, pltpu.VMEM(kv.shape, out_dtype)],
        input_output_aliases={} if first else {len(args) + 1: 0},
        compiler_params=params(20),
        cost_estimate=cost(5 * 2 * rows * width * HEAD_SIZE * 2, 4 * kv.size),
        name="chunk",
    )(where, order, *args)


def finish_kernel(acc, dq_own, dq_send):
    half = dq_own.shape[0] // 2
    width = RATIO * half
    for b in range(4):
        out = dq_own if b < 2 else dq_send
        for h in range(RATIO):
            c = b * width + h * half
            block = (acc[:, c : c + half] * SCALE).T.astype(out.dtype)
            out[(b % 2) * half : (b % 2 + 1) * half, h * HEAD_SIZE : (h + 1) * HEAD_SIZE] = block


def finish(acc, tok, cols):
    out = pltpu.VMEM((tok, cols), jnp.bfloat16)
    return pl.pallas_call(
        finish_kernel,
        in_specs=[VMEM],
        out_specs=[VMEM] * 2,
        out_shape=[out, out],
        compiler_params=params(8),
        cost_estimate=cost(1e6, 6 * acc.size),
        name="finish_q",
    )(near(acc))


def place_kernel(where, mine, theirs, out):
    cols = mine.shape[1]

    @pl.when(where[1] == 0)
    def _():
        out[:, :cols] = mine[...]
        out[:, cols:] = theirs[...]

    @pl.when(where[1] != 0)
    def _():
        out[:, cols:] = mine[...]
        out[:, :cols] = theirs[...]


def place(where, mine, theirs):
    tok, cols = mine.shape
    return pl.pallas_call(
        place_kernel,
        in_specs=[SMEM, VMEM, VMEM],
        out_specs=VMEM,
        out_shape=sds((tok, 2 * cols), mine.dtype),
        compiler_params=params(8),
        cost_estimate=cost(1e6, 8 * mine.size),
        name="place_q",
    )(where, near(mine), near(theirs))


def collect_kernel(n_slots, own, *refs):
    received, outs = refs[: len(refs) - n_slots], refs[len(refs) - n_slots :]
    for s, out in enumerate(outs):
        for j in range(2):
            total = own[j * n_slots + s]
            for r in received:
                total = total + r[j * n_slots + s].astype(jnp.float32)
            out[j] = total.astype(out.dtype)


def collect(own, received):
    n_slots = own.shape[0] // 2
    shape = pltpu.VMEM((2,) + own.shape[1:], jnp.bfloat16)
    return pl.pallas_call(
        functools.partial(collect_kernel, n_slots),
        in_specs=[VMEM] * (1 + len(received)),
        out_specs=[VMEM] * n_slots,
        out_shape=[shape] * n_slots,
        compiler_params=params(8),
        cost_estimate=cost(1e6, 8 * own.size),
        name="collect",
    )(near(own), *[near(r) for r in received])


def unpack_kernel(n, where, *refs):
    core, z = where[1], where[2]
    mine, theirs, dk, dv = refs[:n], refs[n : 2 * n], refs[2 * n], refs[2 * n + 1]
    for m in range(n):
        group = jnp.bitwise_xor(z, m)
        for j, piece in enumerate((mine[m].at[0], theirs[m].at[1])):
            col = (2 * group + jnp.bitwise_xor(core, j)) * HEAD_SIZE
            col = pl.multiple_of(col, HEAD_SIZE)
            dk[:, pl.ds(col, HEAD_SIZE)] = piece[0]
            dv[:, pl.ds(col, HEAD_SIZE)] = piece[1]


def unpack(where, mine, theirs):
    n = len(mine)
    piece = mine[0].shape[2]
    out = sds((piece, KEY_VALUE_HEADS * HEAD_SIZE), jnp.bfloat16)
    return pl.pallas_call(
        functools.partial(unpack_kernel, n),
        in_specs=[SMEM] + [VMEM] * (2 * n),
        out_specs=[VMEM] * 2,
        out_shape=[out] * 2,
        compiler_params=params(8),
        cost_estimate=cost(1e6, 8 * piece * 1024),
        name="unpack_kv",
    )(where, *[near(x) for x in mine], *[near(x) for x in theirs])


def exchange(x, axis, size, m):
    return lax.ppermute(x, axis, [(i, i ^ m) for i in range(size)])


def local(n_chips, n_heads, queries, keys, values, outputs, out_grad, log_norm, block_order):
    where = jnp.stack([lax.axis_index("chip"), lax.axis_index("core"), lax.axis_index("head")])
    tok, cols = queries.shape
    halves = [tuple(m for m in range(n_heads) if m % 2 == a) for a in range(2)]

    zs = pack(where, keys, values, n_heads)
    order = [m for a in halves for m in a if m]
    zr = {0: zs[0]}
    for m in order:
        zr[m] = exchange(zs[m], "head", n_heads, m)
    own_side = prepare(where, queries, out_grad, outputs, log_norm)
    q_side = list(own_side[:3]) + [exchange(x, "core", 2, 1) for x in own_side[3:]]

    kvs = []
    for slots in halves:
        cr = [exchange(zr[m], "core", 2, 1) for m in slots]
        kv = assemble([zr[m] for m in slots], cr)
        kvs.append([kv] + [exchange(kv, "chip", n_chips, m) for m in range(1, n_chips)])

    acc = None
    back, theirs = {}, {}
    for slots, pieces in zip(halves, kvs):
        received = []
        for m in range(n_chips):
            acc, dkv = chunk(
                m, slots, where, block_order, q_side, pieces[m], acc,
                jnp.bfloat16 if m else jnp.float32,
            )
            if m:
                received.append(exchange(dkv, "chip", n_chips, m))
            else:
                own = dkv
        for m, x in zip(slots, collect(own, received)):
            back[m] = exchange(x, "head", n_heads, m) if m else x
            theirs[m] = exchange(back[m], "core", 2, 1)
    dq_own, dq_send = finish(acc, tok, cols // 2)
    dq = place(where, dq_own, exchange(dq_send, "core", 2, 1))
    dk, dv = unpack(where, [back[m] for m in range(n_heads)], [theirs[m] for m in range(n_heads)])
    return dq, dk, dv


def solution(mesh):
    n_seq, n_heads = mesh.shape["seq"], mesh.shape["head"]
    n_chips = n_seq // 2
    fine = Mesh(mesh.devices.reshape(n_chips, 2, n_heads), ("chip", "core", "head"))
    seq = ("chip", "core")
    rows, tokens = P(seq, "head"), P(("chip", "core", "head"), None)
    in_specs = (rows, tokens, tokens, rows, rows, P("head", seq), P())
    out_specs = (rows, tokens, tokens)

    def body(*args):
        return local(n_chips, n_heads, *args)

    return jax.shard_map(body, mesh=fine, in_specs=in_specs, out_specs=out_specs, check_vma=False)
```

```python
import functools

import jax
import jax.numpy as jnp
from jax import lax
from jax.experimental import pallas as pl
from jax.experimental.pallas import tpu as pltpu
from jax.sharding import Mesh
from jax.sharding import PartitionSpec as P


QUERY_HEADS = 32
KEY_VALUE_HEADS = 8
HEAD_SIZE = 128
LOG2E = 1.4426950408889634
SCALE = HEAD_SIZE ** (-0.5)
RATIO = QUERY_HEADS // KEY_VALUE_HEADS


VMEM = pl.BlockSpec(memory_space=pltpu.VMEM)
SMEM = pl.BlockSpec(memory_space=pltpu.SMEM)
ANY = pl.BlockSpec(memory_space=pl.ANY)


def sds(shape, dtype):
    return jax.ShapeDtypeStruct(shape, dtype)


def cost(flops, size):
    return pl.CostEstimate(flops=int(flops), bytes_accessed=int(size), transcendentals=0)


def near(x):
    return pltpu.with_memory_space_constraint(x, pltpu.VMEM)


def params(mib=16):
    return pltpu.CompilerParams(vmem_limit_bytes=mib << 20)


def far(x):
    return pltpu.with_memory_space_constraint(x, pltpu.HBM)


def columns(group):
    return pl.ds(pl.multiple_of(group * HEAD_SIZE, HEAD_SIZE), HEAD_SIZE)


def copy_all(copies, sems):
    started = [pltpu.make_async_copy(src, dst, sems.at[i]) for i, (src, dst) in enumerate(copies)]
    for copy in started:
        copy.start()
    return started


def pack_kernel(where, keys, values, *rest):
    outs, sems = rest[:-1], rest[-1]
    core, z = where[1], where[2]
    copies = []
    for m, out in enumerate(outs):
        group = jnp.bitwise_xor(z, m)
        for j in range(2):
            col = columns(2 * group + jnp.bitwise_xor(core, j))
            copies.append((keys.at[:, col], out.at[j, 0]))
            copies.append((values.at[:, col], out.at[j, 1]))
    for copy in copy_all(copies, sems):
        copy.wait()


def pack(where, keys, values, n_heads):
    shape = (2, 2, keys.shape[0], HEAD_SIZE)
    return pl.pallas_call(
        pack_kernel,
        in_specs=[SMEM, ANY, ANY],
        out_specs=[VMEM] * n_heads,
        out_shape=[pltpu.VMEM(shape, keys.dtype)] * n_heads,
        scratch_shapes=[pltpu.SemaphoreType.DMA((4 * n_heads,))],
        compiler_params=params(8),
        cost_estimate=cost(1e6, 4 * keys.size * 2),
        name="pack_kv",
    )(where, far(keys), far(values))


def prepare_kernel(where, q, do, o, lse, *rest):
    outs, (o_blocks, sems) = rest[:6], rest[6:]
    core = where[1]
    half = q.shape[0] // 2
    copies = []
    for side in range(2):
        first = jnp.bitwise_xor(core, side) * RATIO
        for b in range(2):
            for h in range(RATIO):
                src = (slice(b * half, (b + 1) * half), columns(first + h))
                i = b * RATIO + h
                dst = slice(i * half, (i + 1) * half)
                copies.append((do.at[src], outs[3 * side + 1].at[dst, :]))
                copies.append((o.at[src], o_blocks.at[side, dst, :]))
                copies.append((q.at[src], outs[3 * side].at[dst, :]))
    started = copy_all(copies, sems)
    scaled = lse[...] * LOG2E
    for side in range(2):
        own_low = jnp.bitwise_xor(core, side) == 0
        outs[3 * side + 2][:RATIO, :] = jnp.where(own_low, scaled[:RATIO], scaled[RATIO:])
    for copy in started:
        copy.wait()
    for side in range(2):
        do_ref, stats = outs[3 * side + 1], outs[3 * side + 2]
        for b in range(2):
            for h in range(RATIO):
                i = b * RATIO + h
                rows = slice(i * half, (i + 1) * half)
                prod = do_ref[rows, :].astype(jnp.float32) * o_blocks[side, rows, :].astype(jnp.float32)
                total = jnp.sum(prod.T, axis=0, keepdims=True)
                stats[RATIO + h : RATIO + h + 1, b * half : (b + 1) * half] = total


def prepare(where, q, do, o, lse):
    tok = q.shape[0]
    part = pltpu.VMEM((tok * RATIO, HEAD_SIZE), q.dtype)
    stats = pltpu.VMEM((2 * RATIO, tok), jnp.float32)
    return pl.pallas_call(
        prepare_kernel,
        in_specs=[SMEM, ANY, ANY, ANY, VMEM],
        out_specs=[VMEM] * 6,
        out_shape=[part, part, stats] * 2,
        scratch_shapes=[
            pltpu.VMEM((2, tok * RATIO, HEAD_SIZE), q.dtype),
            pltpu.SemaphoreType.DMA((12 * RATIO,)),
        ],
        compiler_params=params(8),
        cost_estimate=cost(1e7, 8 * q.size),
        name="prepare_q",
    )(where, far(q), far(do), far(o), lse)


def assemble_kernel(n_slots, *refs):
    out = refs[-1]
    for s in range(n_slots):
        out[s] = refs[s][0]
        out[n_slots + s] = refs[n_slots + s][1]


def assemble(mine, theirs):
    n_slots = len(mine)
    shape = (2 * n_slots,) + mine[0].shape[1:]
    return pl.pallas_call(
        functools.partial(assemble_kernel, n_slots),
        in_specs=[VMEM] * (2 * n_slots),
        out_specs=VMEM,
        out_shape=pltpu.VMEM(shape, mine[0].dtype),
        compiler_params=params(8),
        cost_estimate=cost(1e6, 1e6),
        name="assemble",
    )(*[near(x) for x in mine], *[near(x) for x in theirs])


def chunk_kernel(m, slots, n_heads, first, where, q0, do0, stats0, q1, do1, stats1, kv, *rest):
    acc, dkv = rest[-2:]
    c, core, z = where[0], where[1], where[2]
    piece = kv.shape[2]
    half = stats0.shape[1] // 2
    width = RATIO * half
    per_block = half // piece
    other = jnp.bitwise_xor(c, m)
    pieces = []
    for j in range(2):
        for slot in slots:
            source = jnp.bitwise_xor(z, slot)
            block = where[3 + (other * 2 + jnp.bitwise_xor(core, j)) * 2 + source // per_block]
            pieces.append((j * n_heads + slot, block * half + (source % per_block) * piece))
    per_tile = min(len(pieces), 256 // piece)
    tiles = [range(i, i + per_tile) for i in range(0, len(pieces), per_tile)]
    row = lax.broadcasted_iota(jnp.int32, (piece, half), 0)
    lane = lax.broadcasted_iota(jnp.int32, (piece, half), 1)
    offset = jnp.concatenate([row - lane] * per_tile, 0)
    ks = [jnp.concatenate([kv[pieces[p][0], 0] for p in t], 0) for t in tiles]
    vs = [jnp.concatenate([kv[pieces[p][0], 1] for p in t], 0) for t in tiles]
    kts = [k.T for k in ks]
    nt = (((1,), (1,)), ((), ()))
    dks, dvs = [None] * len(tiles), [None] * len(tiles)
    for b in range(4):
        q_ref, do_ref, stats = (q0, do0, stats0) if b < 2 else (q1, do1, stats1)
        i = b % 2
        lo = where[3 + (c * 2 + jnp.bitwise_xor(core, b // 2)) * 2 + i] * half
        qs = q_ref[i * width : (i + 1) * width, :]
        dos = do_ref[i * width : (i + 1) * width, :]
        dq = None if first else rest[0][:, b * width : (b + 1) * width]
        for t, tile in enumerate(tiles):
            s = lax.dot_general(ks[t], qs, nt, preferred_element_type=jnp.float32)
            dp = lax.dot_general(vs[t], dos, nt, preferred_element_type=jnp.float32)
            limits = [jnp.full((piece, half), lo - pieces[p][1], jnp.int32) for p in tile]
            visible = offset <= jnp.concatenate(limits, 0)
            probs, scores = [], []
            for h in range(RATIO):
                cols = slice(h * half, (h + 1) * half)
                lse = stats[h : h + 1, i * half : (i + 1) * half]
                delta = stats[RATIO + h : RATIO + h + 1, i * half : (i + 1) * half]
                p = jnp.where(visible, jnp.exp2(s[:, cols] * (SCALE * LOG2E) - lse), 0.0)
                probs.append(p.astype(jnp.bfloat16))
                scores.append((p * (dp[:, cols] - delta)).astype(jnp.bfloat16))
            prob = jnp.concatenate(probs, 1)
            score = jnp.concatenate(scores, 1)
            dv = jnp.dot(prob, dos, preferred_element_type=jnp.float32)
            dk = jnp.dot(score, qs, preferred_element_type=jnp.float32)
            dvs[t] = dv if dvs[t] is None else dvs[t] + dv
            dks[t] = dk if dks[t] is None else dks[t] + dk
            term = jnp.dot(kts[t], score, preferred_element_type=jnp.float32)
            dq = term if dq is None else dq + term
        acc[:, b * width : (b + 1) * width] = dq
    for t, tile in enumerate(tiles):
        for n, p in enumerate(tile):
            rows = slice(n * piece, (n + 1) * piece)
            dkv[p, 0] = (dks[t][rows] * SCALE).astype(dkv.dtype)
            dkv[p, 1] = dvs[t][rows].astype(dkv.dtype)


def chunk(m, slots, where, q_side, kv, acc, out_dtype):
    first = acc is None
    width = q_side[0].shape[0] * 2
    acc_out = pltpu.VMEM((HEAD_SIZE, width), jnp.float32)
    args = [near(x) for x in q_side] + [near(kv)] + ([] if first else [near(acc)])
    out = (2 * len(slots),) + kv.shape[1:]
    return pl.pallas_call(
        functools.partial(chunk_kernel, m, slots, kv.shape[0] // 2, first),
        in_specs=[SMEM] + [VMEM] * len(args),
        out_specs=[VMEM] * 2,
        out_shape=[acc_out, pltpu.VMEM(out, out_dtype)],
        input_output_aliases={} if first else {len(args): 0},
        compiler_params=params(20),
        cost_estimate=cost(5 * 2 * out[0] * out[2] * width * HEAD_SIZE * 2, 4 * kv.size),
        name="chunk",
    )(where, *args)


def finish_kernel(acc, dq_own, dq_send):
    half = dq_own.shape[0] // 2
    width = RATIO * half
    for b in range(4):
        out = dq_own if b < 2 else dq_send
        for h in range(RATIO):
            c = b * width + h * half
            block = (acc[:, c : c + half] * SCALE).T.astype(out.dtype)
            out[(b % 2) * half : (b % 2 + 1) * half, h * HEAD_SIZE : (h + 1) * HEAD_SIZE] = block


def finish(acc, tok, cols):
    out = pltpu.VMEM((tok, cols), jnp.bfloat16)
    return pl.pallas_call(
        finish_kernel,
        in_specs=[VMEM],
        out_specs=[VMEM] * 2,
        out_shape=[out, out],
        compiler_params=params(8),
        cost_estimate=cost(1e6, 6 * acc.size),
        name="finish_q",
    )(near(acc))


def place_kernel(where, mine, theirs, out):
    cols = mine.shape[1]

    @pl.when(where[1] == 0)
    def _():
        out[:, :cols] = mine[...]
        out[:, cols:] = theirs[...]

    @pl.when(where[1] != 0)
    def _():
        out[:, cols:] = mine[...]
        out[:, :cols] = theirs[...]


def place(where, mine, theirs):
    tok, cols = mine.shape
    return pl.pallas_call(
        place_kernel,
        in_specs=[SMEM, VMEM, VMEM],
        out_specs=VMEM,
        out_shape=sds((tok, 2 * cols), mine.dtype),
        compiler_params=params(8),
        cost_estimate=cost(1e6, 8 * mine.size),
        name="place_q",
    )(where, near(mine), near(theirs))


def collect_kernel(picks, own, *refs):
    n = len(picks[0]) // 2
    received, outs = refs[: len(refs) - n], refs[len(refs) - n :]
    for s, out in enumerate(outs):
        for j in range(2):
            total = own[picks[0][j * n + s]]
            for pick, r in zip(picks[1:], received):
                total = total + r[pick[j * n + s]].astype(jnp.float32)
            out[j] = total.astype(out.dtype)


def collect(picks, own, received):
    n = len(picks[0]) // 2
    shape = pltpu.VMEM((2,) + own.shape[1:], jnp.bfloat16)
    return pl.pallas_call(
        functools.partial(collect_kernel, picks),
        in_specs=[VMEM] * (1 + len(received)),
        out_specs=[VMEM] * n,
        out_shape=[shape] * n,
        compiler_params=params(8),
        cost_estimate=cost(1e6, 8 * own.size),
        name="collect",
    )(near(own), *[near(r) for r in received])


def unpack_kernel(n, where, *refs):
    core, z = where[1], where[2]
    mine, theirs, dk, dv = refs[:n], refs[n : 2 * n], refs[2 * n], refs[2 * n + 1]
    for m in range(n):
        group = jnp.bitwise_xor(z, m)
        for j, piece in enumerate((mine[m].at[0], theirs[m].at[1])):
            col = (2 * group + jnp.bitwise_xor(core, j)) * HEAD_SIZE
            col = pl.multiple_of(col, HEAD_SIZE)
            dk[:, pl.ds(col, HEAD_SIZE)] = piece[0]
            dv[:, pl.ds(col, HEAD_SIZE)] = piece[1]


def unpack(where, mine, theirs):
    n = len(mine)
    piece = mine[0].shape[2]
    out = sds((piece, KEY_VALUE_HEADS * HEAD_SIZE), jnp.bfloat16)
    return pl.pallas_call(
        functools.partial(unpack_kernel, n),
        in_specs=[SMEM] + [VMEM] * (2 * n),
        out_specs=[VMEM] * 2,
        out_shape=[out] * 2,
        compiler_params=params(8),
        cost_estimate=cost(1e6, 8 * piece * 1024),
        name="unpack_kv",
    )(where, *[near(x) for x in mine], *[near(x) for x in theirs])


def exchange(x, axis, size, m):
    return lax.ppermute(x, axis, [(i, i ^ m) for i in range(size)])


def slot_halves(n_heads):
    slots = sorted(range(n_heads), key=lambda m: (m % 2, m))
    return tuple(slots[: n_heads // 2]), tuple(slots[n_heads // 2 :])


def local(n_chips, n_heads, queries, keys, values, outputs, out_grad, log_norm, block_order):
    where = jnp.stack([lax.axis_index("chip"), lax.axis_index("core"), lax.axis_index("head")])
    tok, cols = queries.shape
    info = jnp.concatenate([where, block_order])
    every = tuple(range(n_heads))
    halves = slot_halves(n_heads)

    zs = pack(where, keys, values, n_heads)
    zr = {0: zs[0]}
    for m in range(1, n_heads):
        zr[m] = exchange(zs[m], "head", n_heads, m)
    own_side = prepare(where, queries, out_grad, outputs, log_norm)
    q_side = list(own_side[:3]) + [exchange(x, "core", 2, 1) for x in own_side[3:]]

    kv = assemble([zr[m] for m in every], [exchange(zr[m], "core", 2, 1) for m in every])
    kvs = [kv]
    for m in range(1, n_chips):
        kvs.append(exchange(kv, "chip", n_chips, m))

    acc = None
    received = []
    for m in range(n_chips - 1):
        acc, dkv = chunk(
            m, every, info, q_side, kvs[m], acc,
            jnp.bfloat16 if m else jnp.float32,
        )
        if m:
            received.append(exchange(dkv, "chip", n_chips, m))
        else:
            own = dkv
    late = []
    m = n_chips - 1
    for slots in halves:
        acc, dkv = chunk(m, slots, info, q_side, kvs[m], acc, jnp.bfloat16)
        late.append(exchange(dkv, "chip", n_chips, m))

    dq_own, dq_send = finish(acc, tok, cols // 2)
    dq_other = exchange(dq_send, "core", 2, 1)
    dq = place(where, dq_own, dq_other)

    back, theirs = {}, {}
    for a, slots in enumerate(halves):
        full = [j * n_heads + slot for j in range(2) for slot in slots]
        picks = [full] * (n_chips - 1) + [list(range(len(full)))]
        sums = collect(picks, own, received + [late[a]])
        for slot, x in zip(slots, sums):
            back[slot] = exchange(x, "head", n_heads, slot) if slot else x
            theirs[slot] = exchange(back[slot], "core", 2, 1)
    dk, dv = unpack(where, [back[m] for m in every], [theirs[m] for m in every])
    return dq, dk, dv


def solution(mesh):
    n_seq, n_heads = mesh.shape["seq"], mesh.shape["head"]
    n_chips = n_seq // 2
    fine = Mesh(mesh.devices.reshape(n_chips, 2, n_heads), ("chip", "core", "head"))
    seq = ("chip", "core")
    rows, tokens = P(seq, "head"), P(("chip", "core", "head"), None)
    in_specs = (rows, tokens, tokens, rows, rows, P("head", seq), P())
    out_specs = (rows, tokens, tokens)

    def body(*args):
        return local(n_chips, n_heads, *args)

    return jax.shard_map(body, mesh=fine, in_specs=in_specs, out_specs=out_specs, check_vma=False)
```

```python
import functools

import jax
import jax.numpy as jnp
from jax import lax
from jax.experimental import pallas as pl
from jax.experimental.pallas import tpu as pltpu
from jax.sharding import Mesh
from jax.sharding import PartitionSpec as P


QUERY_HEADS = 32
KEY_VALUE_HEADS = 8
HEAD_SIZE = 128
LOG2E = 1.4426950408889634
SCALE = HEAD_SIZE ** (-0.5)
RATIO = QUERY_HEADS // KEY_VALUE_HEADS


VMEM = pl.BlockSpec(memory_space=pltpu.VMEM)
SMEM = pl.BlockSpec(memory_space=pltpu.SMEM)
ANY = pl.BlockSpec(memory_space=pl.ANY)


def sds(shape, dtype):
    return jax.ShapeDtypeStruct(shape, dtype)


def cost(flops, size):
    return pl.CostEstimate(flops=int(flops), bytes_accessed=int(size), transcendentals=0)


def near(x):
    return pltpu.with_memory_space_constraint(x, pltpu.VMEM)


def params(mib=16):
    return pltpu.CompilerParams(vmem_limit_bytes=mib << 20)


def far(x):
    return pltpu.with_memory_space_constraint(x, pltpu.HBM)


def columns(group):
    return pl.ds(pl.multiple_of(group * HEAD_SIZE, HEAD_SIZE), HEAD_SIZE)


def copy_all(copies, sems):
    started = [pltpu.make_async_copy(src, dst, sems.at[i]) for i, (src, dst) in enumerate(copies)]
    for copy in started:
        copy.start()
    return started


def pack_kernel(where, keys, values, *rest):
    outs, sems = rest[:-1], rest[-1]
    core, z = where[1], where[2]
    copies = []
    for m, out in enumerate(outs):
        group = jnp.bitwise_xor(z, m)
        for j in range(2):
            col = columns(2 * group + jnp.bitwise_xor(core, j))
            copies.append((keys.at[:, col], out.at[j, 0]))
            copies.append((values.at[:, col], out.at[j, 1]))
    for copy in copy_all(copies, sems):
        copy.wait()


def pack(where, keys, values, n_heads):
    shape = (2, 2, keys.shape[0], HEAD_SIZE)
    return pl.pallas_call(
        pack_kernel,
        in_specs=[SMEM, ANY, ANY],
        out_specs=[VMEM] * n_heads,
        out_shape=[pltpu.VMEM(shape, keys.dtype)] * n_heads,
        scratch_shapes=[pltpu.SemaphoreType.DMA((4 * n_heads,))],
        compiler_params=params(8),
        cost_estimate=cost(1e6, 4 * keys.size * 2),
        name="pack_kv",
    )(where, far(keys), far(values))


def prepare_kernel(where, q, do, o, lse, *rest):
    outs, (o_blocks, sems) = rest[:6], rest[6:]
    core = where[1]
    half = q.shape[0] // 2
    copies = []
    for side in range(2):
        first = jnp.bitwise_xor(core, side) * RATIO
        for b in range(2):
            for h in range(RATIO):
                src = (slice(b * half, (b + 1) * half), columns(first + h))
                i = b * RATIO + h
                dst = slice(i * half, (i + 1) * half)
                copies.append((do.at[src], outs[3 * side + 1].at[dst, :]))
                copies.append((o.at[src], o_blocks.at[side, dst, :]))
                copies.append((q.at[src], outs[3 * side].at[dst, :]))
    started = copy_all(copies, sems)
    scaled = lse[...] * LOG2E
    for side in range(2):
        own_low = jnp.bitwise_xor(core, side) == 0
        outs[3 * side + 2][:RATIO, :] = jnp.where(own_low, scaled[:RATIO], scaled[RATIO:])
    for copy in started:
        copy.wait()
    for side in range(2):
        do_ref, stats = outs[3 * side + 1], outs[3 * side + 2]
        for b in range(2):
            for h in range(RATIO):
                i = b * RATIO + h
                rows = slice(i * half, (i + 1) * half)
                prod = do_ref[rows, :].astype(jnp.float32) * o_blocks[side, rows, :].astype(jnp.float32)
                total = jnp.sum(prod.T, axis=0, keepdims=True)
                stats[RATIO + h : RATIO + h + 1, b * half : (b + 1) * half] = total


def prepare(where, q, do, o, lse):
    tok = q.shape[0]
    part = pltpu.VMEM((tok * RATIO, HEAD_SIZE), q.dtype)
    stats = pltpu.VMEM((2 * RATIO, tok), jnp.float32)
    return pl.pallas_call(
        prepare_kernel,
        in_specs=[SMEM, ANY, ANY, ANY, VMEM],
        out_specs=[VMEM] * 6,
        out_shape=[part, part, stats] * 2,
        scratch_shapes=[
            pltpu.VMEM((2, tok * RATIO, HEAD_SIZE), q.dtype),
            pltpu.SemaphoreType.DMA((12 * RATIO,)),
        ],
        compiler_params=params(8),
        cost_estimate=cost(1e7, 8 * q.size),
        name="prepare_q",
    )(where, far(q), far(do), far(o), lse)


def assemble_kernel(n, refs):
    mine, theirs, out = refs[:n], refs[n : 2 * n], refs[2 * n]
    for s in range(n):
        out[s] = mine[s][0]
        out[n + s] = theirs[s][1]


def assemble(mine, theirs):
    n = len(mine)
    shape = (2 * n,) + mine[0].shape[1:]
    return pl.pallas_call(
        lambda *refs: assemble_kernel(n, refs),
        in_specs=[VMEM] * (2 * n),
        out_specs=VMEM,
        out_shape=pltpu.VMEM(shape, mine[0].dtype),
        compiler_params=params(8),
        cost_estimate=cost(1e6, 1e6),
        name="assemble",
    )(*[near(x) for x in mine], *[near(x) for x in theirs])


def chunk_kernel(m, picks, first, where, q0, do0, stats0, q1, do1, stats1, *rest):
    acc, dkv = rest[-2:]
    n_kv = max(p[0] for p in picks) + 1
    kvs, rest = rest[:n_kv], rest[n_kv:]
    c, core, z = where[0], where[1], where[2]
    piece = kvs[0].shape[2]
    half = stats0.shape[1] // 2
    width = RATIO * half
    per_block = half // piece
    other = jnp.bitwise_xor(c, m)
    pieces = []
    for array, place, j, slot in picks:
        source = jnp.bitwise_xor(z, slot)
        block = where[3 + (other * 2 + jnp.bitwise_xor(core, j)) * 2 + source // per_block]
        pieces.append((kvs[array].at[place], block * half + (source % per_block) * piece))
    per_tile = min(len(pieces), 256 // piece)
    tiles = [range(i, i + per_tile) for i in range(0, len(pieces), per_tile)]
    row = lax.broadcasted_iota(jnp.int32, (piece, half), 0)
    lane = lax.broadcasted_iota(jnp.int32, (piece, half), 1)
    offset = jnp.concatenate([row - lane] * per_tile, 0)
    ks = [jnp.concatenate([pieces[p][0][0] for p in t], 0) for t in tiles]
    vs = [jnp.concatenate([pieces[p][0][1] for p in t], 0) for t in tiles]
    kts = [k.T for k in ks]
    nt = (((1,), (1,)), ((), ()))
    dks, dvs = [None] * len(tiles), [None] * len(tiles)
    for b in range(4):
        q_ref, do_ref, stats = (q0, do0, stats0) if b < 2 else (q1, do1, stats1)
        i = b % 2
        lo = where[3 + (c * 2 + jnp.bitwise_xor(core, b // 2)) * 2 + i] * half
        qs = q_ref[i * width : (i + 1) * width, :]
        dos = do_ref[i * width : (i + 1) * width, :]
        dq = None if first else rest[0][:, b * width : (b + 1) * width]
        for t, tile in enumerate(tiles):
            s = lax.dot_general(ks[t], qs, nt, preferred_element_type=jnp.float32)
            dp = lax.dot_general(vs[t], dos, nt, preferred_element_type=jnp.float32)
            limits = [jnp.full((piece, half), lo - pieces[p][1], jnp.int32) for p in tile]
            visible = offset <= jnp.concatenate(limits, 0)
            probs, scores = [], []
            for h in range(RATIO):
                cols = slice(h * half, (h + 1) * half)
                lse = stats[h : h + 1, i * half : (i + 1) * half]
                delta = stats[RATIO + h : RATIO + h + 1, i * half : (i + 1) * half]
                p = jnp.where(visible, jnp.exp2(s[:, cols] * (SCALE * LOG2E) - lse), 0.0)
                probs.append(p.astype(jnp.bfloat16))
                scores.append((p * (dp[:, cols] - delta)).astype(jnp.bfloat16))
            prob = jnp.concatenate(probs, 1)
            score = jnp.concatenate(scores, 1)
            dv = jnp.dot(prob, dos, preferred_element_type=jnp.float32)
            dk = jnp.dot(score, qs, preferred_element_type=jnp.float32)
            dvs[t] = dv if dvs[t] is None else dvs[t] + dv
            dks[t] = dk if dks[t] is None else dks[t] + dk
            term = jnp.dot(kts[t], score, preferred_element_type=jnp.float32)
            dq = term if dq is None else dq + term
        acc[:, b * width : (b + 1) * width] = dq
    for t, tile in enumerate(tiles):
        for n, p in enumerate(tile):
            rows = slice(n * piece, (n + 1) * piece)
            dkv[p, 0] = (dks[t][rows] * SCALE).astype(dkv.dtype)
            dkv[p, 1] = dvs[t][rows].astype(dkv.dtype)


def chunk(m, picks, where, q_side, kvs, acc, out_dtype):
    first = acc is None
    width = q_side[0].shape[0] * 2
    acc_out = pltpu.VMEM((HEAD_SIZE, width), jnp.float32)
    args = [near(x) for x in q_side] + [near(kv) for kv in kvs] + ([] if first else [near(acc)])
    out = (len(picks),) + kvs[0].shape[1:]
    return pl.pallas_call(
        functools.partial(chunk_kernel, m, picks, first),
        in_specs=[SMEM] + [VMEM] * len(args),
        out_specs=[VMEM] * 2,
        out_shape=[acc_out, pltpu.VMEM(out, out_dtype)],
        input_output_aliases={} if first else {len(args): 0},
        compiler_params=params(20),
        cost_estimate=cost(5 * 2 * out[0] * out[2] * width * HEAD_SIZE * 2, 4 * kvs[0].size),
        name="chunk",
    )(where, *args)


def finish_kernel(acc, dq_own, dq_send):
    half = dq_own.shape[0] // 2
    width = RATIO * half
    for b in range(4):
        out = dq_own if b < 2 else dq_send
        for h in range(RATIO):
            c = b * width + h * half
            block = (acc[:, c : c + half] * SCALE).T.astype(out.dtype)
            out[(b % 2) * half : (b % 2 + 1) * half, h * HEAD_SIZE : (h + 1) * HEAD_SIZE] = block


def finish(acc, tok, cols):
    out = pltpu.VMEM((tok, cols), jnp.bfloat16)
    return pl.pallas_call(
        finish_kernel,
        in_specs=[VMEM],
        out_specs=[VMEM] * 2,
        out_shape=[out, out],
        compiler_params=params(8),
        cost_estimate=cost(1e6, 6 * acc.size),
        name="finish_q",
    )(near(acc))


def place_kernel(where, mine, theirs, out):
    cols = mine.shape[1]

    @pl.when(where[1] == 0)
    def _():
        out[:, :cols] = mine[...]
        out[:, cols:] = theirs[...]

    @pl.when(where[1] != 0)
    def _():
        out[:, cols:] = mine[...]
        out[:, :cols] = theirs[...]


def place(where, mine, theirs):
    tok, cols = mine.shape
    return pl.pallas_call(
        place_kernel,
        in_specs=[SMEM, VMEM, VMEM],
        out_specs=VMEM,
        out_shape=sds((tok, 2 * cols), mine.dtype),
        compiler_params=params(8),
        cost_estimate=cost(1e6, 8 * mine.size),
        name="place_q",
    )(where, near(mine), near(theirs))


def collect_kernel(picks, own, *refs):
    n = len(picks[0]) // 2
    received, outs = refs[: len(refs) - n], refs[len(refs) - n :]
    for s, out in enumerate(outs):
        for j in range(2):
            total = own[picks[0][j * n + s]]
            for pick, r in zip(picks[1:], received):
                total = total + r[pick[j * n + s]].astype(jnp.float32)
            out[j] = total.astype(out.dtype)


def collect(picks, own, received):
    n = len(picks[0]) // 2
    shape = pltpu.VMEM((2,) + own.shape[1:], jnp.bfloat16)
    return pl.pallas_call(
        functools.partial(collect_kernel, picks),
        in_specs=[VMEM] * (1 + len(received)),
        out_specs=[VMEM] * n,
        out_shape=[shape] * n,
        compiler_params=params(8),
        cost_estimate=cost(1e6, 8 * own.size),
        name="collect",
    )(near(own), *[near(r) for r in received])


def unpack_kernel(n, where, *refs):
    core, z = where[1], where[2]
    mine, theirs, dk, dv = refs[:n], refs[n : 2 * n], refs[2 * n], refs[2 * n + 1]
    for m in range(n):
        group = jnp.bitwise_xor(z, m)
        for j, piece in enumerate((mine[m].at[0], theirs[m].at[1])):
            col = (2 * group + jnp.bitwise_xor(core, j)) * HEAD_SIZE
            col = pl.multiple_of(col, HEAD_SIZE)
            dk[:, pl.ds(col, HEAD_SIZE)] = piece[0]
            dv[:, pl.ds(col, HEAD_SIZE)] = piece[1]


def unpack(where, mine, theirs):
    n = len(mine)
    piece = mine[0].shape[2]
    out = sds((piece, KEY_VALUE_HEADS * HEAD_SIZE), jnp.bfloat16)
    return pl.pallas_call(
        functools.partial(unpack_kernel, n),
        in_specs=[SMEM] + [VMEM] * (2 * n),
        out_specs=[VMEM] * 2,
        out_shape=[out] * 2,
        compiler_params=params(8),
        cost_estimate=cost(1e6, 8 * piece * 1024),
        name="unpack_kv",
    )(where, *[near(x) for x in mine], *[near(x) for x in theirs])


def exchange(x, axis, size, m):
    return lax.ppermute(x, axis, [(i, i ^ m) for i in range(size)])


def slot_halves(n_heads):
    slots = sorted(range(n_heads), key=lambda m: (m % 2, m))
    return tuple(slots[: n_heads // 2]), tuple(slots[n_heads // 2 :])


def local(n_chips, n_heads, queries, keys, values, outputs, out_grad, log_norm, block_order):
    where = jnp.stack([lax.axis_index("chip"), lax.axis_index("core"), lax.axis_index("head")])
    tok, cols = queries.shape
    info = jnp.concatenate([where, block_order])
    every = tuple(range(n_heads))
    halves = slot_halves(n_heads)

    zs = pack(where, keys, values, n_heads)
    zr = {0: zs[0]}
    for m in range(1, n_heads):
        zr[m] = exchange(zs[m], "head", n_heads, m)
    own_side = prepare(where, queries, out_grad, outputs, log_norm)
    q_side = list(own_side[:3]) + [exchange(x, "core", 2, 1) for x in own_side[3:]]

    other = {}
    for m in every:
        other[m] = exchange(zr[m], "core", 2, 1)
    last = n_chips - 1
    own, sent = [], [[] for _ in range(n_chips)]
    for a, slots in enumerate(halves):
        own.append(assemble([zr[m] for m in slots], [other[m] for m in slots]))
        for m in range(1, last):
            sent[m].append(exchange(own[a], "chip", n_chips, m))
    full = [m for slots in halves for m in slots]
    whole = assemble([zr[m] for m in full], [other[m] for m in full])
    far_kv = exchange(whole, "chip", n_chips, last)

    half_picks = [
        (a, j * len(slots) + i, j, slot)
        for a, slots in enumerate(halves)
        for j in range(2)
        for i, slot in enumerate(slots)
    ]
    far_picks = [
        [(0, j * n_heads + full.index(slot), j, slot) for j in range(2) for slot in slots]
        for slots in halves
    ]
    acc = None
    received, late = [], []
    for m in range(1, last):
        acc, dkv = chunk(m, half_picks, info, q_side, sent[m], acc, jnp.bfloat16)
        received.append(exchange(dkv, "chip", n_chips, m))
    for a in range(2):
        acc, dkv = chunk(last, far_picks[a], info, q_side, [far_kv], acc, jnp.bfloat16)
        late.append(exchange(dkv, "chip", n_chips, last))
    acc, total = chunk(0, half_picks, info, q_side, own, acc, jnp.float32)

    dq_own, dq_send = finish(acc, tok, cols // 2)
    dq_other = exchange(dq_send, "core", 2, 1)
    dq = place(where, dq_own, dq_other)

    back, theirs = {}, {}
    for a, slots in enumerate(halves):
        n = 2 * len(slots)
        picks = [[i for i, p in enumerate(half_picks) if p[0] == a]] * last + [list(range(n))]
        sums = collect(picks, total, received + [late[a]])
        for slot, x in zip(slots, sums):
            back[slot] = exchange(x, "head", n_heads, slot) if slot else x
            theirs[slot] = exchange(back[slot], "core", 2, 1)
    dk, dv = unpack(where, [back[m] for m in every], [theirs[m] for m in every])
    return dq, dk, dv


def solution(mesh):
    n_seq, n_heads = mesh.shape["seq"], mesh.shape["head"]
    n_chips = n_seq // 2
    fine = Mesh(mesh.devices.reshape(n_chips, 2, n_heads), ("chip", "core", "head"))
    seq = ("chip", "core")
    rows, tokens = P(seq, "head"), P(("chip", "core", "head"), None)
    in_specs = (rows, tokens, tokens, rows, rows, P("head", seq), P())
    out_specs = (rows, tokens, tokens)

    def body(*args):
        return local(n_chips, n_heads, *args)

    return jax.shard_map(body, mesh=fine, in_specs=in_specs, out_specs=out_specs, check_vma=False)
```

```python
import functools

import jax
import jax.numpy as jnp
from jax import lax
from jax.experimental import pallas as pl
from jax.experimental.pallas import tpu as pltpu
from jax.sharding import Mesh
from jax.sharding import PartitionSpec as P


QUERY_HEADS = 32
KEY_VALUE_HEADS = 8
HEAD_SIZE = 128
LOG2E = 1.4426950408889634
SCALE = HEAD_SIZE ** (-0.5)
RATIO = QUERY_HEADS // KEY_VALUE_HEADS


VMEM = pl.BlockSpec(memory_space=pltpu.VMEM)
SMEM = pl.BlockSpec(memory_space=pltpu.SMEM)
ANY = pl.BlockSpec(memory_space=pl.ANY)


def sds(shape, dtype):
    return jax.ShapeDtypeStruct(shape, dtype)


def cost(flops, size):
    return pl.CostEstimate(flops=int(flops), bytes_accessed=int(size), transcendentals=0)


def near(x):
    return pltpu.with_memory_space_constraint(x, pltpu.VMEM)


def params(mib=16):
    return pltpu.CompilerParams(vmem_limit_bytes=mib << 20)


def far(x):
    return pltpu.with_memory_space_constraint(x, pltpu.HBM)


def columns(group):
    return pl.ds(pl.multiple_of(group * HEAD_SIZE, HEAD_SIZE), HEAD_SIZE)


def copy_all(copies, sems):
    started = [pltpu.make_async_copy(src, dst, sems.at[i]) for i, (src, dst) in enumerate(copies)]
    for copy in started:
        copy.start()
    return started


def pack_kernel(where, keys, values, *rest):
    outs, sems = rest[:-1], rest[-1]
    core, z = where[1], where[2]
    copies = []
    for m, out in enumerate(outs):
        group = jnp.bitwise_xor(z, m)
        for j in range(2):
            col = columns(2 * group + jnp.bitwise_xor(core, j))
            copies.append((keys.at[:, col], out.at[j, 0]))
            copies.append((values.at[:, col], out.at[j, 1]))
    for copy in copy_all(copies, sems):
        copy.wait()


def pack(where, keys, values, n_heads):
    shape = (2, 2, keys.shape[0], HEAD_SIZE)
    return pl.pallas_call(
        pack_kernel,
        in_specs=[SMEM, ANY, ANY],
        out_specs=[VMEM] * n_heads,
        out_shape=[pltpu.VMEM(shape, keys.dtype)] * n_heads,
        scratch_shapes=[pltpu.SemaphoreType.DMA((4 * n_heads,))],
        compiler_params=params(8),
        cost_estimate=cost(1e6, 4 * keys.size * 2),
        name="pack_kv",
    )(where, far(keys), far(values))


def prepare_kernel(where, q, do, o, lse, *rest):
    outs, (o_blocks, sems) = rest[:6], rest[6:]
    core = where[1]
    half = q.shape[0] // 2
    copies = []
    for side in range(2):
        first = jnp.bitwise_xor(core, side) * RATIO
        for b in range(2):
            for h in range(RATIO):
                src = (slice(b * half, (b + 1) * half), columns(first + h))
                i = b * RATIO + h
                dst = slice(i * half, (i + 1) * half)
                copies.append((do.at[src], outs[3 * side + 1].at[dst, :]))
                copies.append((o.at[src], o_blocks.at[side, dst, :]))
                copies.append((q.at[src], outs[3 * side].at[dst, :]))
    started = copy_all(copies, sems)
    scaled = lse[...] * LOG2E
    for side in range(2):
        own_low = jnp.bitwise_xor(core, side) == 0
        outs[3 * side + 2][:RATIO, :] = jnp.where(own_low, scaled[:RATIO], scaled[RATIO:])
    for copy in started:
        copy.wait()
    for side in range(2):
        do_ref, stats = outs[3 * side + 1], outs[3 * side + 2]
        for b in range(2):
            for h in range(RATIO):
                i = b * RATIO + h
                rows = slice(i * half, (i + 1) * half)
                prod = do_ref[rows, :].astype(jnp.float32) * o_blocks[side, rows, :].astype(jnp.float32)
                total = jnp.sum(prod.T, axis=0, keepdims=True)
                stats[RATIO + h : RATIO + h + 1, b * half : (b + 1) * half] = total


def prepare(where, q, do, o, lse):
    tok = q.shape[0]
    part = pltpu.VMEM((tok * RATIO, HEAD_SIZE), q.dtype)
    stats = pltpu.VMEM((2 * RATIO, tok), jnp.float32)
    return pl.pallas_call(
        prepare_kernel,
        in_specs=[SMEM, ANY, ANY, ANY, VMEM],
        out_specs=[VMEM] * 6,
        out_shape=[part, part, stats] * 2,
        scratch_shapes=[
            pltpu.VMEM((2, tok * RATIO, HEAD_SIZE), q.dtype),
            pltpu.SemaphoreType.DMA((12 * RATIO,)),
        ],
        compiler_params=params(8),
        cost_estimate=cost(1e7, 8 * q.size),
        name="prepare_q",
    )(where, far(q), far(do), far(o), lse)


def assemble_kernel(n, refs):
    mine, theirs, out = refs[:n], refs[n : 2 * n], refs[2 * n]
    for s in range(n):
        out[s] = mine[s][0]
        out[n + s] = theirs[s][1]


def assemble(mine, theirs):
    n = len(mine)
    shape = (2 * n,) + mine[0].shape[1:]
    return pl.pallas_call(
        lambda *refs: assemble_kernel(n, refs),
        in_specs=[VMEM] * (2 * n),
        out_specs=VMEM,
        out_shape=pltpu.VMEM(shape, mine[0].dtype),
        compiler_params=params(8),
        cost_estimate=cost(1e6, 1e6),
        name="assemble",
    )(*[near(x) for x in mine], *[near(x) for x in theirs])


def chunk_kernel(m, groups, first, where, q0, do0, stats0, q1, do1, stats1, *rest):
    acc, dkvs = rest[-1 - len(groups)], rest[-len(groups) :]
    picks = [p for group in groups for p in group]
    n_kv = max(p[0] for p in picks) + 1
    kvs, rest = rest[:n_kv], rest[n_kv:]
    c, core, z = where[0], where[1], where[2]
    piece = kvs[0].shape[2]
    half = stats0.shape[1] // 2
    width = RATIO * half
    per_block = half // piece
    other = jnp.bitwise_xor(c, m)
    pieces = []
    for array, place, j, slot in picks:
        source = jnp.bitwise_xor(z, slot)
        block = where[3 + (other * 2 + jnp.bitwise_xor(core, j)) * 2 + source // per_block]
        pieces.append((kvs[array].at[place], block * half + (source % per_block) * piece))
    per_tile = min(len(pieces), 256 // piece)
    tiles = [range(i, i + per_tile) for i in range(0, len(pieces), per_tile)]
    row = lax.broadcasted_iota(jnp.int32, (piece, half), 0)
    lane = lax.broadcasted_iota(jnp.int32, (piece, half), 1)
    offset = jnp.concatenate([row - lane] * per_tile, 0)
    ks = [jnp.concatenate([pieces[p][0][0] for p in t], 0) for t in tiles]
    vs = [jnp.concatenate([pieces[p][0][1] for p in t], 0) for t in tiles]
    kts = [k.T for k in ks]
    nt = (((1,), (1,)), ((), ()))
    dks, dvs = [None] * len(tiles), [None] * len(tiles)
    for b in range(4):
        q_ref, do_ref, stats = (q0, do0, stats0) if b < 2 else (q1, do1, stats1)
        i = b % 2
        lo = where[3 + (c * 2 + jnp.bitwise_xor(core, b // 2)) * 2 + i] * half
        qs = q_ref[i * width : (i + 1) * width, :]
        dos = do_ref[i * width : (i + 1) * width, :]
        dq = None if first else rest[0][:, b * width : (b + 1) * width]
        for t, tile in enumerate(tiles):
            s = lax.dot_general(ks[t], qs, nt, preferred_element_type=jnp.float32)
            dp = lax.dot_general(vs[t], dos, nt, preferred_element_type=jnp.float32)
            limits = [jnp.full((piece, half), lo - pieces[p][1], jnp.int32) for p in tile]
            visible = offset <= jnp.concatenate(limits, 0)
            probs, scores = [], []
            for h in range(RATIO):
                cols = slice(h * half, (h + 1) * half)
                lse = stats[h : h + 1, i * half : (i + 1) * half]
                delta = stats[RATIO + h : RATIO + h + 1, i * half : (i + 1) * half]
                p = jnp.where(visible, jnp.exp2(s[:, cols] * (SCALE * LOG2E) - lse), 0.0)
                probs.append(p.astype(jnp.bfloat16))
                scores.append((p * (dp[:, cols] - delta)).astype(jnp.bfloat16))
            prob = jnp.concatenate(probs, 1)
            score = jnp.concatenate(scores, 1)
            dv = jnp.dot(prob, dos, preferred_element_type=jnp.float32)
            dk = jnp.dot(score, qs, preferred_element_type=jnp.float32)
            dvs[t] = dv if dvs[t] is None else dvs[t] + dv
            dks[t] = dk if dks[t] is None else dks[t] + dk
            term = jnp.dot(kts[t], score, preferred_element_type=jnp.float32)
            dq = term if dq is None else dq + term
        acc[:, b * width : (b + 1) * width] = dq
    targets = [dkv.at[i] for dkv, group in zip(dkvs, groups) for i in range(len(group))]
    for t, tile in enumerate(tiles):
        for n, p in enumerate(tile):
            rows = slice(n * piece, (n + 1) * piece)
            targets[p][0] = (dks[t][rows] * SCALE).astype(targets[p].dtype)
            targets[p][1] = dvs[t][rows].astype(targets[p].dtype)


def chunk(m, groups, where, q_side, kvs, acc, out_dtype):
    first = acc is None
    width = q_side[0].shape[0] * 2
    acc_out = pltpu.VMEM((HEAD_SIZE, width), jnp.float32)
    args = [near(x) for x in q_side] + [near(kv) for kv in kvs] + ([] if first else [near(acc)])
    outs = [pltpu.VMEM((len(g),) + kvs[0].shape[1:], out_dtype) for g in groups]
    rows = sum(len(g) for g in groups) * kvs[0].shape[2]
    return pl.pallas_call(
        functools.partial(chunk_kernel, m, groups, first),
        in_specs=[SMEM] + [VMEM] * len(args),
        out_specs=[VMEM] * (1 + len(outs)),
        out_shape=[acc_out] + outs,
        input_output_aliases={} if first else {len(args): 0},
        compiler_params=params(20),
        cost_estimate=cost(5 * 2 * rows * width * HEAD_SIZE * 2, 4 * kvs[0].size),
        name="chunk",
    )(where, *args)


def finish_kernel(acc, dq_own, dq_send):
    half = dq_own.shape[0] // 2
    width = RATIO * half
    for b in range(4):
        out = dq_own if b < 2 else dq_send
        for h in range(RATIO):
            c = b * width + h * half
            block = (acc[:, c : c + half] * SCALE).T.astype(out.dtype)
            out[(b % 2) * half : (b % 2 + 1) * half, h * HEAD_SIZE : (h + 1) * HEAD_SIZE] = block


def finish(acc, tok, cols):
    out = pltpu.VMEM((tok, cols), jnp.bfloat16)
    return pl.pallas_call(
        finish_kernel,
        in_specs=[VMEM],
        out_specs=[VMEM] * 2,
        out_shape=[out, out],
        compiler_params=params(8),
        cost_estimate=cost(1e6, 6 * acc.size),
        name="finish_q",
    )(near(acc))


def place_kernel(where, mine, theirs, out):
    cols = mine.shape[1]

    @pl.when(where[1] == 0)
    def _():
        out[:, :cols] = mine[...]
        out[:, cols:] = theirs[...]

    @pl.when(where[1] != 0)
    def _():
        out[:, cols:] = mine[...]
        out[:, :cols] = theirs[...]


def place(where, mine, theirs):
    tok, cols = mine.shape
    return pl.pallas_call(
        place_kernel,
        in_specs=[SMEM, VMEM, VMEM],
        out_specs=VMEM,
        out_shape=sds((tok, 2 * cols), mine.dtype),
        compiler_params=params(8),
        cost_estimate=cost(1e6, 8 * mine.size),
        name="place_q",
    )(where, near(mine), near(theirs))


def collect_kernel(picks, own, *refs):
    n = len(picks[0]) // 2
    received, outs = refs[: len(refs) - n], refs[len(refs) - n :]
    for s, out in enumerate(outs):
        for j in range(2):
            total = own[picks[0][j * n + s]]
            for pick, r in zip(picks[1:], received):
                total = total + r[pick[j * n + s]].astype(jnp.float32)
            out[j] = total.astype(out.dtype)


def collect(picks, own, received):
    n = len(picks[0]) // 2
    shape = pltpu.VMEM((2,) + own.shape[1:], jnp.bfloat16)
    return pl.pallas_call(
        functools.partial(collect_kernel, picks),
        in_specs=[VMEM] * (1 + len(received)),
        out_specs=[VMEM] * n,
        out_shape=[shape] * n,
        compiler_params=params(8),
        cost_estimate=cost(1e6, 8 * own.size),
        name="collect",
    )(near(own), *[near(r) for r in received])


def unpack_kernel(n, where, *refs):
    core, z = where[1], where[2]
    mine, theirs, dk, dv = refs[:n], refs[n : 2 * n], refs[2 * n], refs[2 * n + 1]
    for m in range(n):
        group = jnp.bitwise_xor(z, m)
        for j, piece in enumerate((mine[m].at[0], theirs[m].at[1])):
            col = (2 * group + jnp.bitwise_xor(core, j)) * HEAD_SIZE
            col = pl.multiple_of(col, HEAD_SIZE)
            dk[:, pl.ds(col, HEAD_SIZE)] = piece[0]
            dv[:, pl.ds(col, HEAD_SIZE)] = piece[1]


def unpack(where, mine, theirs):
    n = len(mine)
    piece = mine[0].shape[2]
    out = sds((piece, KEY_VALUE_HEADS * HEAD_SIZE), jnp.bfloat16)
    return pl.pallas_call(
        functools.partial(unpack_kernel, n),
        in_specs=[SMEM] + [VMEM] * (2 * n),
        out_specs=[VMEM] * 2,
        out_shape=[out] * 2,
        compiler_params=params(8),
        cost_estimate=cost(1e6, 8 * piece * 1024),
        name="unpack_kv",
    )(where, *[near(x) for x in mine], *[near(x) for x in theirs])


def exchange(x, axis, size, m):
    return lax.ppermute(x, axis, [(i, i ^ m) for i in range(size)])


def slot_halves(n_heads):
    slots = sorted(range(n_heads), key=lambda m: (m % 2, m))
    return tuple(slots[: n_heads // 2]), tuple(slots[n_heads // 2 :])


def home_halves(n_heads):
    return tuple(range(n_heads // 2, n_heads)), tuple(range(n_heads // 2))


def local(n_chips, n_heads, queries, keys, values, outputs, out_grad, log_norm, block_order):
    where = jnp.stack([lax.axis_index("chip"), lax.axis_index("core"), lax.axis_index("head")])
    tok, cols = queries.shape
    info = jnp.concatenate([where, block_order])
    every = tuple(range(n_heads))
    halves = slot_halves(n_heads)

    zs = pack(where, keys, values, n_heads)
    zr = {0: zs[0]}
    for m in range(1, n_heads):
        zr[m] = exchange(zs[m], "head", n_heads, m)
    own_side = prepare(where, queries, out_grad, outputs, log_norm)
    q_side = list(own_side[:3]) + [exchange(x, "core", 2, 1) for x in own_side[3:]]

    other = {}
    for m in every:
        other[m] = exchange(zr[m], "core", 2, 1)
    last = n_chips - 1
    own, sent = [], [[] for _ in range(n_chips)]
    for a, slots in enumerate(halves):
        own.append(assemble([zr[m] for m in slots], [other[m] for m in slots]))
        for m in range(1, last):
            sent[m].append(exchange(own[a], "chip", n_chips, m))
    for a, (first, second) in enumerate(((1, last ^ 1), (last ^ 1, 1))):
        sent[last].append(exchange(sent[first][a], "chip", n_chips, second))

    half_picks = [
        (a, j * len(slots) + i, j, slot)
        for a, slots in enumerate(halves)
        for j in range(2)
        for i, slot in enumerate(slots)
    ]
    home = home_halves(n_heads)
    home_picks = [[p for p in half_picks if p[3] in slots] for slots in home]
    acc = None
    total, received, late = [], [], [[], []]
    acc, dkv = chunk(0, home_picks[:1], info, q_side, own, acc, jnp.float32)
    total.append(dkv)
    for m in range(1, n_chips):
        groups = [half_picks] if m < last - 1 else home_picks
        acc, *parts = chunk(m, groups, info, q_side, sent[m], acc, jnp.bfloat16)
        for a, dkv in enumerate(parts):
            dkv = exchange(dkv, "chip", n_chips, m)
            (received if m < last - 1 else late[a]).append(dkv)
    acc, dkv = chunk(0, home_picks[1:], info, q_side, own, acc, jnp.float32)
    total.append(dkv)

    dq_own, dq_send = finish(acc, tok, cols // 2)
    dq_other = exchange(dq_send, "core", 2, 1)
    dq = place(where, dq_own, dq_other)

    back, theirs = {}, {}
    for a, slots in enumerate(home):
        wanted = [(j, slot) for j in range(2) for slot in slots]
        part = [[p[2:] for p in home_picks[a]].index(w) for w in wanted]
        full = [[p[2:] for p in half_picks].index(w) for w in wanted]
        picks = [part] + [full] * len(received) + [part] * len(late[a])
        sums = collect(picks, total[a], received + late[a])
        for slot, x in zip(slots, sums):
            back[slot] = exchange(x, "head", n_heads, slot) if slot else x
            theirs[slot] = exchange(back[slot], "core", 2, 1)
    dk, dv = unpack(where, [back[m] for m in every], [theirs[m] for m in every])
    return dq, dk, dv


def solution(mesh):
    n_seq, n_heads = mesh.shape["seq"], mesh.shape["head"]
    n_chips = n_seq // 2
    fine = Mesh(mesh.devices.reshape(n_chips, 2, n_heads), ("chip", "core", "head"))
    seq = ("chip", "core")
    rows, tokens = P(seq, "head"), P(("chip", "core", "head"), None)
    in_specs = (rows, tokens, tokens, rows, rows, P("head", seq), P())
    out_specs = (rows, tokens, tokens)

    def body(*args):
        return local(n_chips, n_heads, *args)

    return jax.shard_map(body, mesh=fine, in_specs=in_specs, out_specs=out_specs, check_vma=False)
```

```python
import functools

import jax
import jax.numpy as jnp
from jax import lax
from jax.experimental import pallas as pl
from jax.experimental.pallas import tpu as pltpu
from jax.sharding import Mesh
from jax.sharding import PartitionSpec as P


QUERY_HEADS = 32
KEY_VALUE_HEADS = 8
HEAD_SIZE = 128
LOG2E = 1.4426950408889634
SCALE = HEAD_SIZE ** (-0.5)
RATIO = QUERY_HEADS // KEY_VALUE_HEADS


VMEM = pl.BlockSpec(memory_space=pltpu.VMEM)
SMEM = pl.BlockSpec(memory_space=pltpu.SMEM)
ANY = pl.BlockSpec(memory_space=pl.ANY)


def sds(shape, dtype):
    return jax.ShapeDtypeStruct(shape, dtype)


def cost(flops, size):
    return pl.CostEstimate(flops=int(flops), bytes_accessed=int(size), transcendentals=0)


def near(x):
    return pltpu.with_memory_space_constraint(x, pltpu.VMEM)


def params(mib=16):
    return pltpu.CompilerParams(vmem_limit_bytes=mib << 20)


def far(x):
    return pltpu.with_memory_space_constraint(x, pltpu.HBM)


def columns(group):
    return pl.ds(pl.multiple_of(group * HEAD_SIZE, HEAD_SIZE), HEAD_SIZE)


def copy_all(copies, sems):
    started = [pltpu.make_async_copy(src, dst, sems.at[i]) for i, (src, dst) in enumerate(copies)]
    for copy in started:
        copy.start()
    return started


def pack_kernel(where, keys, values, *rest):
    outs, sems = rest[:-1], rest[-1]
    core, z = where[1], where[2]
    copies = []
    for m, out in enumerate(outs):
        group = jnp.bitwise_xor(z, m)
        for j in range(2):
            col = columns(2 * group + jnp.bitwise_xor(core, j))
            copies.append((keys.at[:, col], out.at[j, 0]))
            copies.append((values.at[:, col], out.at[j, 1]))
    for copy in copy_all(copies, sems):
        copy.wait()


def pack(where, keys, values, n_heads):
    shape = (2, 2, keys.shape[0], HEAD_SIZE)
    return pl.pallas_call(
        pack_kernel,
        in_specs=[SMEM, ANY, ANY],
        out_specs=[VMEM] * n_heads,
        out_shape=[pltpu.VMEM(shape, keys.dtype)] * n_heads,
        scratch_shapes=[pltpu.SemaphoreType.DMA((4 * n_heads,))],
        compiler_params=params(8),
        cost_estimate=cost(1e6, 4 * keys.size * 2),
        name="pack_kv",
    )(where, far(keys), far(values))


def prepare_kernel(where, q, do, o, lse, *rest):
    outs, (o_blocks, sems) = rest[:6], rest[6:]
    core = where[1]
    half = q.shape[0] // 2
    copies = []
    for side in range(2):
        first = jnp.bitwise_xor(core, side) * RATIO
        for b in range(2):
            for h in range(RATIO):
                src = (slice(b * half, (b + 1) * half), columns(first + h))
                i = b * RATIO + h
                dst = slice(i * half, (i + 1) * half)
                copies.append((do.at[src], outs[3 * side + 1].at[dst, :]))
                copies.append((o.at[src], o_blocks.at[side, dst, :]))
                copies.append((q.at[src], outs[3 * side].at[dst, :]))
    started = copy_all(copies, sems)
    scaled = lse[...] * LOG2E
    for side in range(2):
        own_low = jnp.bitwise_xor(core, side) == 0
        outs[3 * side + 2][:RATIO, :] = jnp.where(own_low, scaled[:RATIO], scaled[RATIO:])
    for copy in started:
        copy.wait()
    for side in range(2):
        do_ref, stats = outs[3 * side + 1], outs[3 * side + 2]
        for b in range(2):
            for h in range(RATIO):
                i = b * RATIO + h
                rows = slice(i * half, (i + 1) * half)
                prod = do_ref[rows, :].astype(jnp.float32) * o_blocks[side, rows, :].astype(jnp.float32)
                total = jnp.sum(prod.T, axis=0, keepdims=True)
                stats[RATIO + h : RATIO + h + 1, b * half : (b + 1) * half] = total


def prepare(where, q, do, o, lse):
    tok = q.shape[0]
    part = pltpu.VMEM((tok * RATIO, HEAD_SIZE), q.dtype)
    stats = pltpu.VMEM((2 * RATIO, tok), jnp.float32)
    return pl.pallas_call(
        prepare_kernel,
        in_specs=[SMEM, ANY, ANY, ANY, VMEM],
        out_specs=[VMEM] * 6,
        out_shape=[part, part, stats] * 2,
        scratch_shapes=[
            pltpu.VMEM((2, tok * RATIO, HEAD_SIZE), q.dtype),
            pltpu.SemaphoreType.DMA((12 * RATIO,)),
        ],
        compiler_params=params(8),
        cost_estimate=cost(1e7, 8 * q.size),
        name="prepare_q",
    )(where, far(q), far(do), far(o), lse)


def assemble_kernel(n, refs):
    mine, theirs, out = refs[:n], refs[n : 2 * n], refs[2 * n]
    for s in range(n):
        out[s] = mine[s][0]
        out[n + s] = theirs[s][1]


def assemble(mine, theirs):
    n = len(mine)
    shape = (2 * n,) + mine[0].shape[1:]
    return pl.pallas_call(
        lambda *refs: assemble_kernel(n, refs),
        in_specs=[VMEM] * (2 * n),
        out_specs=VMEM,
        out_shape=pltpu.VMEM(shape, mine[0].dtype),
        compiler_params=params(8),
        cost_estimate=cost(1e6, 1e6),
        name="assemble",
    )(*[near(x) for x in mine], *[near(x) for x in theirs])


def chunk_kernel(m, groups, first, where, q0, do0, stats0, q1, do1, stats1, *rest):
    dk_acc, dv_acc = rest[-2:]
    rest = rest[:-2]
    acc, dkvs = rest[-1 - len(groups)], rest[-len(groups) :]
    picks = [p for group in groups for p in group]
    n_kv = max(p[0] for p in picks) + 1
    kvs, rest = rest[:n_kv], rest[n_kv:]
    c, core, z = where[0], where[1], where[2]
    piece = kvs[0].shape[2]
    half = stats0.shape[1] // 2
    width = RATIO * half
    per_block = half // piece
    other = jnp.bitwise_xor(c, m)
    pieces = []
    for array, place, j, slot in picks:
        source = jnp.bitwise_xor(z, slot)
        block = where[3 + (other * 2 + jnp.bitwise_xor(core, j)) * 2 + source // per_block]
        pieces.append((kvs[array].at[place], block * half + (source % per_block) * piece))
    per_tile = min(len(pieces), 256 // piece)
    tiles = [range(i, i + per_tile) for i in range(0, len(pieces), per_tile)]
    row = lax.broadcasted_iota(jnp.int32, (piece, half), 0)
    lane = lax.broadcasted_iota(jnp.int32, (piece, half), 1)
    offset = jnp.concatenate([row - lane] * per_tile, 0)
    ks = [jnp.concatenate([pieces[p][0][0] for p in t], 0) for t in tiles]
    vs = [jnp.concatenate([pieces[p][0][1] for p in t], 0) for t in tiles]
    kts = [k.T for k in ks]
    nt = (((1,), (1,)), ((), ()))
    for b in range(4):
        q_ref, do_ref, stats = (q0, do0, stats0) if b < 2 else (q1, do1, stats1)
        i = b % 2
        lo = where[3 + (c * 2 + jnp.bitwise_xor(core, b // 2)) * 2 + i] * half
        qs = q_ref[i * width : (i + 1) * width, :]
        dos = do_ref[i * width : (i + 1) * width, :]
        dq = None if first else rest[0][:, b * width : (b + 1) * width]
        for t, tile in enumerate(tiles):
            s = lax.dot_general(ks[t], qs, nt, preferred_element_type=jnp.float32)
            dp = lax.dot_general(vs[t], dos, nt, preferred_element_type=jnp.float32)
            limits = [jnp.full((piece, half), lo - pieces[p][1], jnp.int32) for p in tile]
            visible = offset <= jnp.concatenate(limits, 0)
            probs, scores = [], []
            for h in range(RATIO):
                cols = slice(h * half, (h + 1) * half)
                lse = stats[h : h + 1, i * half : (i + 1) * half]
                delta = stats[RATIO + h : RATIO + h + 1, i * half : (i + 1) * half]
                p = jnp.where(visible, jnp.exp2(s[:, cols] * (SCALE * LOG2E) - lse), 0.0)
                probs.append(p.astype(jnp.bfloat16))
                scores.append((p * (dp[:, cols] - delta)).astype(jnp.bfloat16))
            prob = jnp.concatenate(probs, 1)
            score = jnp.concatenate(scores, 1)
            dv = jnp.dot(prob, dos, preferred_element_type=jnp.float32)
            dk = jnp.dot(score, qs, preferred_element_type=jnp.float32)
            span = slice(t * per_tile * piece, (t + 1) * per_tile * piece)
            if b == 0:
                dv_acc[span, :] = dv
                dk_acc[span, :] = dk
            else:
                dv_acc[span, :] += dv
                dk_acc[span, :] += dk
            term = jnp.dot(kts[t], score, preferred_element_type=jnp.float32)
            dq = term if dq is None else dq + term
        acc[:, b * width : (b + 1) * width] = dq
    targets = [dkv.at[i] for dkv, group in zip(dkvs, groups) for i in range(len(group))]
    for tile in tiles:
        for p in tile:
            rows = slice(p * piece, (p + 1) * piece)
            targets[p][0] = (dk_acc[rows, :] * SCALE).astype(targets[p].dtype)
            targets[p][1] = dv_acc[rows, :].astype(targets[p].dtype)


def chunk(m, groups, where, q_side, kvs, acc, out_dtype):
    first = acc is None
    width = q_side[0].shape[0] * 2
    acc_out = pltpu.VMEM((HEAD_SIZE, width), jnp.float32)
    args = [near(x) for x in q_side] + [near(kv) for kv in kvs] + ([] if first else [near(acc)])
    outs = [pltpu.VMEM((len(g),) + kvs[0].shape[1:], out_dtype) for g in groups]
    rows = sum(len(g) for g in groups) * kvs[0].shape[2]
    return pl.pallas_call(
        functools.partial(chunk_kernel, m, groups, first),
        in_specs=[SMEM] + [VMEM] * len(args),
        out_specs=[VMEM] * (1 + len(outs)),
        out_shape=[acc_out] + outs,
        input_output_aliases={} if first else {len(args): 0},
        scratch_shapes=[pltpu.VMEM((rows, HEAD_SIZE), jnp.float32)] * 2,
        compiler_params=params(20),
        cost_estimate=cost(5 * 2 * rows * width * HEAD_SIZE * 2, 4 * kvs[0].size),
        name="chunk",
    )(where, *args)


def finish_kernel(acc, dq_own, dq_send):
    half = dq_own.shape[0] // 2
    width = RATIO * half
    for b in range(4):
        out = dq_own if b < 2 else dq_send
        for h in range(RATIO):
            c = b * width + h * half
            block = (acc[:, c : c + half] * SCALE).T.astype(out.dtype)
            out[(b % 2) * half : (b % 2 + 1) * half, h * HEAD_SIZE : (h + 1) * HEAD_SIZE] = block


def finish(acc, tok, cols):
    out = pltpu.VMEM((tok, cols), jnp.bfloat16)
    return pl.pallas_call(
        finish_kernel,
        in_specs=[VMEM],
        out_specs=[VMEM] * 2,
        out_shape=[out, out],
        compiler_params=params(8),
        cost_estimate=cost(1e6, 6 * acc.size),
        name="finish_q",
    )(near(acc))


def place_kernel(where, mine, theirs, out):
    cols = mine.shape[1]

    @pl.when(where[1] == 0)
    def _():
        out[:, :cols] = mine[...]
        out[:, cols:] = theirs[...]

    @pl.when(where[1] != 0)
    def _():
        out[:, cols:] = mine[...]
        out[:, :cols] = theirs[...]


def place(where, mine, theirs):
    tok, cols = mine.shape
    return pl.pallas_call(
        place_kernel,
        in_specs=[SMEM, VMEM, VMEM],
        out_specs=VMEM,
        out_shape=sds((tok, 2 * cols), mine.dtype),
        compiler_params=params(8),
        cost_estimate=cost(1e6, 8 * mine.size),
        name="place_q",
    )(where, near(mine), near(theirs))


def collect_kernel(picks, own, *refs):
    n = len(picks[0]) // 2
    received, outs = refs[: len(refs) - n], refs[len(refs) - n :]
    for s, out in enumerate(outs):
        for j in range(2):
            total = own[picks[0][j * n + s]]
            for pick, r in zip(picks[1:], received):
                total = total + r[pick[j * n + s]].astype(jnp.float32)
            out[j] = total.astype(out.dtype)


def collect(picks, own, received):
    n = len(picks[0]) // 2
    shape = pltpu.VMEM((2,) + own.shape[1:], jnp.bfloat16)
    return pl.pallas_call(
        functools.partial(collect_kernel, picks),
        in_specs=[VMEM] * (1 + len(received)),
        out_specs=[VMEM] * n,
        out_shape=[shape] * n,
        compiler_params=params(8),
        cost_estimate=cost(1e6, 8 * own.size),
        name="collect",
    )(near(own), *[near(r) for r in received])


def unpack_kernel(n, where, *refs):
    core, z = where[1], where[2]
    mine, theirs, dk, dv = refs[:n], refs[n : 2 * n], refs[2 * n], refs[2 * n + 1]
    for m in range(n):
        group = jnp.bitwise_xor(z, m)
        for j, piece in enumerate((mine[m].at[0], theirs[m].at[1])):
            col = (2 * group + jnp.bitwise_xor(core, j)) * HEAD_SIZE
            col = pl.multiple_of(col, HEAD_SIZE)
            dk[:, pl.ds(col, HEAD_SIZE)] = piece[0]
            dv[:, pl.ds(col, HEAD_SIZE)] = piece[1]


def unpack(where, mine, theirs):
    n = len(mine)
    piece = mine[0].shape[2]
    out = sds((piece, KEY_VALUE_HEADS * HEAD_SIZE), jnp.bfloat16)
    return pl.pallas_call(
        functools.partial(unpack_kernel, n),
        in_specs=[SMEM] + [VMEM] * (2 * n),
        out_specs=[VMEM] * 2,
        out_shape=[out] * 2,
        compiler_params=params(8),
        cost_estimate=cost(1e6, 8 * piece * 1024),
        name="unpack_kv",
    )(where, *[near(x) for x in mine], *[near(x) for x in theirs])


def exchange(x, axis, size, m):
    return lax.ppermute(x, axis, [(i, i ^ m) for i in range(size)])


def slot_halves(n_heads):
    slots = sorted(range(n_heads), key=lambda m: (m % 2, m))
    return tuple(slots[: n_heads // 2]), tuple(slots[n_heads // 2 :])


def home_halves(n_heads):
    return tuple(range(n_heads // 2, n_heads)), tuple(range(n_heads // 2))


def local(n_chips, n_heads, queries, keys, values, outputs, out_grad, log_norm, block_order):
    where = jnp.stack([lax.axis_index("chip"), lax.axis_index("core"), lax.axis_index("head")])
    tok, cols = queries.shape
    info = jnp.concatenate([where, block_order])
    every = tuple(range(n_heads))
    halves = slot_halves(n_heads)

    zs = pack(where, keys, values, n_heads)
    zr = {0: zs[0]}
    for m in range(1, n_heads):
        zr[m] = exchange(zs[m], "head", n_heads, m)
    own_side = prepare(where, queries, out_grad, outputs, log_norm)
    q_side = list(own_side[:3]) + [exchange(x, "core", 2, 1) for x in own_side[3:]]

    other = {}
    for m in every:
        other[m] = exchange(zr[m], "core", 2, 1)
    last = n_chips - 1
    near_chips = list(range(last - 1, 0, -1))
    own, sent = [], [[] for _ in range(n_chips)]
    for a, slots in enumerate(halves):
        own.append(assemble([zr[m] for m in slots], [other[m] for m in slots]))
        for m in near_chips:
            sent[m].append(exchange(own[a], "chip", n_chips, m))
    full = halves[0] + halves[1]
    whole = assemble([zr[m] for m in full], [other[m] for m in full])
    sent[last].append(exchange(whole, "chip", n_chips, last))

    half_picks = [
        (a, j * len(slots) + i, j, slot)
        for a, slots in enumerate(halves)
        for j in range(2)
        for i, slot in enumerate(slots)
    ]
    home = home_halves(n_heads)
    home_picks = [[p for p in half_picks if p[3] in slots] for slots in home]
    far_picks = [[(0, j * n_heads + full.index(slot), j, slot) for _, _, j, slot in g] for g in home_picks]
    acc = None
    total, received, late = [], [], [[], []]
    acc, dkv = chunk(0, home_picks[:1], info, q_side, own, acc, jnp.float32)
    total.append(dkv)
    for m in near_chips + [last]:
        groups = far_picks if m == last else home_picks if m == near_chips[-1] else [half_picks]
        acc, *parts = chunk(m, groups, info, q_side, sent[m], acc, jnp.bfloat16)
        for a, dkv in enumerate(parts):
            dkv = exchange(dkv, "chip", n_chips, m)
            (received if len(parts) == 1 else late[a]).append(dkv)
    acc, dkv = chunk(0, home_picks[1:], info, q_side, own, acc, jnp.float32)
    total.append(dkv)

    dq_own, dq_send = finish(acc, tok, cols // 2)
    dq_other = exchange(dq_send, "core", 2, 1)
    dq = place(where, dq_own, dq_other)

    back, theirs = {}, {}
    for a, slots in enumerate(home):
        wanted = [(j, slot) for j in range(2) for slot in slots]
        part = [[p[2:] for p in home_picks[a]].index(w) for w in wanted]
        full = [[p[2:] for p in half_picks].index(w) for w in wanted]
        picks = [part] + [full] * len(received) + [part] * len(late[a])
        sums = collect(picks, total[a], received + late[a])
        for slot, x in zip(slots, sums):
            back[slot] = exchange(x, "head", n_heads, slot) if slot else x
            theirs[slot] = exchange(back[slot], "core", 2, 1)
    dk, dv = unpack(where, [back[m] for m in every], [theirs[m] for m in every])
    return dq, dk, dv


def solution(mesh):
    n_seq, n_heads = mesh.shape["seq"], mesh.shape["head"]
    n_chips = n_seq // 2
    fine = Mesh(mesh.devices.reshape(n_chips, 2, n_heads), ("chip", "core", "head"))
    seq = ("chip", "core")
    rows, tokens = P(seq, "head"), P(("chip", "core", "head"), None)
    in_specs = (rows, tokens, tokens, rows, rows, P("head", seq), P())
    out_specs = (rows, tokens, tokens)

    def body(*args):
        return local(n_chips, n_heads, *args)

    return jax.shard_map(body, mesh=fine, in_specs=in_specs, out_specs=out_specs, check_vma=False)
```

```python
import functools

import jax
import jax.numpy as jnp
from jax import lax
from jax.experimental import pallas as pl
from jax.experimental.pallas import tpu as pltpu
from jax.sharding import Mesh
from jax.sharding import PartitionSpec as P


QUERY_HEADS = 32
KEY_VALUE_HEADS = 8
HEAD_SIZE = 128
LOG2E = 1.4426950408889634
SCALE = HEAD_SIZE ** (-0.5)
RATIO = QUERY_HEADS // KEY_VALUE_HEADS


VMEM = pl.BlockSpec(memory_space=pltpu.VMEM)
SMEM = pl.BlockSpec(memory_space=pltpu.SMEM)
ANY = pl.BlockSpec(memory_space=pl.ANY)


def sds(shape, dtype):
    return jax.ShapeDtypeStruct(shape, dtype)


def cost(flops, size):
    return pl.CostEstimate(flops=int(flops), bytes_accessed=int(size), transcendentals=0)


def near(x):
    return pltpu.with_memory_space_constraint(x, pltpu.VMEM)


def params(mib=16):
    return pltpu.CompilerParams(vmem_limit_bytes=mib << 20)


def far(x):
    return pltpu.with_memory_space_constraint(x, pltpu.HBM)


def columns(group):
    return pl.ds(pl.multiple_of(group * HEAD_SIZE, HEAD_SIZE), HEAD_SIZE)


def copy_all(copies, sems):
    started = [pltpu.make_async_copy(src, dst, sems.at[i]) for i, (src, dst) in enumerate(copies)]
    for copy in started:
        copy.start()
    return started


def pack_kernel(where, keys, values, *rest):
    outs, sems = rest[:-1], rest[-1]
    core, z = where[1], where[2]
    copies = []
    for m, out in enumerate(outs):
        group = jnp.bitwise_xor(z, m)
        for j in range(2):
            col = columns(2 * group + jnp.bitwise_xor(core, j))
            copies.append((keys.at[:, col], out.at[j, 0]))
            copies.append((values.at[:, col], out.at[j, 1]))
    for copy in copy_all(copies, sems):
        copy.wait()


def pack(where, keys, values, n_heads):
    shape = (2, 2, keys.shape[0], HEAD_SIZE)
    return pl.pallas_call(
        pack_kernel,
        in_specs=[SMEM, ANY, ANY],
        out_specs=[VMEM] * n_heads,
        out_shape=[pltpu.VMEM(shape, keys.dtype)] * n_heads,
        scratch_shapes=[pltpu.SemaphoreType.DMA((4 * n_heads,))],
        compiler_params=params(8),
        cost_estimate=cost(1e6, 4 * keys.size * 2),
        name="pack_kv",
    )(where, far(keys), far(values))


def prepare_kernel(where, q, do, o, lse, *rest):
    outs, (o_blocks, sems) = rest[:6], rest[6:]
    core = where[1]
    half = q.shape[0] // 2
    copies = []
    for side in range(2):
        first = jnp.bitwise_xor(core, side) * RATIO
        for b in range(2):
            for h in range(RATIO):
                src = (slice(b * half, (b + 1) * half), columns(first + h))
                i = b * RATIO + h
                dst = slice(i * half, (i + 1) * half)
                copies.append((do.at[src], outs[3 * side + 1].at[dst, :]))
                copies.append((o.at[src], o_blocks.at[side, dst, :]))
                copies.append((q.at[src], outs[3 * side].at[dst, :]))
    started = copy_all(copies, sems)
    scaled = lse[...] * LOG2E
    for side in range(2):
        own_low = jnp.bitwise_xor(core, side) == 0
        outs[3 * side + 2][:RATIO, :] = jnp.where(own_low, scaled[:RATIO], scaled[RATIO:])
    for copy in started:
        copy.wait()
    for side in range(2):
        do_ref, stats = outs[3 * side + 1], outs[3 * side + 2]
        for b in range(2):
            for h in range(RATIO):
                i = b * RATIO + h
                rows = slice(i * half, (i + 1) * half)
                prod = do_ref[rows, :].astype(jnp.float32) * o_blocks[side, rows, :].astype(jnp.float32)
                total = jnp.sum(prod.T, axis=0, keepdims=True)
                stats[RATIO + h : RATIO + h + 1, b * half : (b + 1) * half] = total


def prepare(where, q, do, o, lse):
    tok = q.shape[0]
    part = pltpu.VMEM((tok * RATIO, HEAD_SIZE), q.dtype)
    stats = pltpu.VMEM((2 * RATIO, tok), jnp.float32)
    return pl.pallas_call(
        prepare_kernel,
        in_specs=[SMEM, ANY, ANY, ANY, VMEM],
        out_specs=[VMEM] * 6,
        out_shape=[part, part, stats] * 2,
        scratch_shapes=[
            pltpu.VMEM((2, tok * RATIO, HEAD_SIZE), q.dtype),
            pltpu.SemaphoreType.DMA((12 * RATIO,)),
        ],
        compiler_params=params(8),
        cost_estimate=cost(1e7, 8 * q.size),
        name="prepare_q",
    )(where, far(q), far(do), far(o), lse)


def assemble_kernel(n, refs):
    mine, theirs, out = refs[:n], refs[n : 2 * n], refs[2 * n]
    for s in range(n):
        out[s] = mine[s][0]
        out[n + s] = theirs[s][1]


def assemble(mine, theirs):
    n = len(mine)
    shape = (2 * n,) + mine[0].shape[1:]
    return pl.pallas_call(
        lambda *refs: assemble_kernel(n, refs),
        in_specs=[VMEM] * (2 * n),
        out_specs=VMEM,
        out_shape=pltpu.VMEM(shape, mine[0].dtype),
        compiler_params=params(8),
        cost_estimate=cost(1e6, 1e6),
        name="assemble",
    )(*[near(x) for x in mine], *[near(x) for x in theirs])


def chunk_kernel(m, groups, first, where, q0, do0, stats0, q1, do1, stats1, *rest):
    dk_acc, dv_acc = rest[-2:]
    rest = rest[:-2]
    acc, dkvs = rest[-1 - len(groups)], rest[-len(groups) :]
    picks = [p for group in groups for p in group]
    n_kv = max(p[0] for p in picks) + 1
    kvs, rest = rest[:n_kv], rest[n_kv:]
    c, core, z = where[0], where[1], where[2]
    piece = kvs[0].shape[2]
    half = stats0.shape[1] // 2
    width = RATIO * half
    per_block = half // piece
    other = jnp.bitwise_xor(c, m)
    pieces = []
    for array, place, j, slot in picks:
        source = jnp.bitwise_xor(z, slot)
        block = where[3 + (other * 2 + jnp.bitwise_xor(core, j)) * 2 + source // per_block]
        pieces.append((kvs[array].at[place], block * half + (source % per_block) * piece))
    per_tile = min(len(pieces), 256 // piece)
    tiles = [range(i, i + per_tile) for i in range(0, len(pieces), per_tile)]
    row = lax.broadcasted_iota(jnp.int32, (piece, half), 0)
    lane = lax.broadcasted_iota(jnp.int32, (piece, half), 1)
    offset = jnp.concatenate([row - lane] * per_tile, 0)
    ks = [jnp.concatenate([pieces[p][0][0] for p in t], 0) for t in tiles]
    vs = [jnp.concatenate([pieces[p][0][1] for p in t], 0) for t in tiles]
    kts = [k.T for k in ks]
    nt = (((1,), (1,)), ((), ()))
    for b in range(4):
        q_ref, do_ref, stats = (q0, do0, stats0) if b < 2 else (q1, do1, stats1)
        i = b % 2
        lo = where[3 + (c * 2 + jnp.bitwise_xor(core, b // 2)) * 2 + i] * half
        qs = q_ref[i * width : (i + 1) * width, :]
        dos = do_ref[i * width : (i + 1) * width, :]
        dq = None if first else rest[0][:, b * width : (b + 1) * width]
        for t, tile in enumerate(tiles):
            s = lax.dot_general(ks[t], qs, nt, preferred_element_type=jnp.float32)
            dp = lax.dot_general(vs[t], dos, nt, preferred_element_type=jnp.float32)
            limits = [jnp.full((piece, half), lo - pieces[p][1], jnp.int32) for p in tile]
            visible = offset <= jnp.concatenate(limits, 0)
            probs, scores = [], []
            for h in range(RATIO):
                cols = slice(h * half, (h + 1) * half)
                lse = stats[h : h + 1, i * half : (i + 1) * half]
                delta = stats[RATIO + h : RATIO + h + 1, i * half : (i + 1) * half]
                p = jnp.where(visible, jnp.exp2(s[:, cols] * (SCALE * LOG2E) - lse), 0.0)
                probs.append(p.astype(jnp.bfloat16))
                scores.append((p * (dp[:, cols] - delta)).astype(jnp.bfloat16))
            prob = jnp.concatenate(probs, 1)
            score = jnp.concatenate(scores, 1)
            dv = jnp.dot(prob, dos, preferred_element_type=jnp.float32)
            dk = jnp.dot(score, qs, preferred_element_type=jnp.float32)
            span = slice(t * per_tile * piece, (t + 1) * per_tile * piece)
            if b == 0:
                dv_acc[span, :] = dv
                dk_acc[span, :] = dk
            else:
                dv_acc[span, :] += dv
                dk_acc[span, :] += dk
            term = jnp.dot(kts[t], score, preferred_element_type=jnp.float32)
            dq = term if dq is None else dq + term
        acc[:, b * width : (b + 1) * width] = dq
    targets = [dkv.at[i] for dkv, group in zip(dkvs, groups) for i in range(len(group))]
    for tile in tiles:
        for p in tile:
            rows = slice(p * piece, (p + 1) * piece)
            targets[p][0] = (dk_acc[rows, :] * SCALE).astype(targets[p].dtype)
            targets[p][1] = dv_acc[rows, :].astype(targets[p].dtype)


def chunk(m, groups, where, q_side, kvs, acc, out_dtype):
    first = acc is None
    width = q_side[0].shape[0] * 2
    acc_out = pltpu.VMEM((HEAD_SIZE, width), jnp.float32)
    args = [near(x) for x in q_side] + [near(kv) for kv in kvs] + ([] if first else [near(acc)])
    outs = [pltpu.VMEM((len(g),) + kvs[0].shape[1:], out_dtype) for g in groups]
    rows = sum(len(g) for g in groups) * kvs[0].shape[2]
    return pl.pallas_call(
        functools.partial(chunk_kernel, m, groups, first),
        in_specs=[SMEM] + [VMEM] * len(args),
        out_specs=[VMEM] * (1 + len(outs)),
        out_shape=[acc_out] + outs,
        input_output_aliases={} if first else {len(args): 0},
        scratch_shapes=[pltpu.VMEM((rows, HEAD_SIZE), jnp.float32)] * 2,
        compiler_params=params(20),
        cost_estimate=cost(5 * 2 * rows * width * HEAD_SIZE * 2, 4 * kvs[0].size),
        name="chunk",
    )(where, *args)


def finish_kernel(acc, dq_own, dq_send):
    half = dq_own.shape[0] // 2
    width = RATIO * half
    for b in range(4):
        out = dq_own if b < 2 else dq_send
        for h in range(RATIO):
            c = b * width + h * half
            block = (acc[:, c : c + half] * SCALE).T.astype(out.dtype)
            out[(b % 2) * half : (b % 2 + 1) * half, h * HEAD_SIZE : (h + 1) * HEAD_SIZE] = block


def finish(acc, tok, cols):
    out = pltpu.VMEM((tok, cols), jnp.bfloat16)
    return pl.pallas_call(
        finish_kernel,
        in_specs=[VMEM],
        out_specs=[VMEM] * 2,
        out_shape=[out, out],
        compiler_params=params(8),
        cost_estimate=cost(1e6, 6 * acc.size),
        name="finish_q",
    )(near(acc))


def place_kernel(where, mine, theirs, out):
    cols = mine.shape[1]

    @pl.when(where[1] == 0)
    def _():
        out[:, :cols] = mine[...]
        out[:, cols:] = theirs[...]

    @pl.when(where[1] != 0)
    def _():
        out[:, cols:] = mine[...]
        out[:, :cols] = theirs[...]


def place(where, mine, theirs):
    tok, cols = mine.shape
    return pl.pallas_call(
        place_kernel,
        in_specs=[SMEM, VMEM, VMEM],
        out_specs=VMEM,
        out_shape=sds((tok, 2 * cols), mine.dtype),
        compiler_params=params(8),
        cost_estimate=cost(1e6, 8 * mine.size),
        name="place_q",
    )(where, near(mine), near(theirs))


def collect_kernel(picks, own, *refs):
    n = len(picks[0]) // 2
    received, outs = refs[: len(refs) - n], refs[len(refs) - n :]
    for s, out in enumerate(outs):
        for j in range(2):
            total = own[picks[0][j * n + s]]
            for pick, r in zip(picks[1:], received):
                total = total + r[pick[j * n + s]].astype(jnp.float32)
            out[j] = total.astype(out.dtype)


def collect(picks, own, received):
    n = len(picks[0]) // 2
    shape = pltpu.VMEM((2,) + own.shape[1:], jnp.bfloat16)
    return pl.pallas_call(
        functools.partial(collect_kernel, picks),
        in_specs=[VMEM] * (1 + len(received)),
        out_specs=[VMEM] * n,
        out_shape=[shape] * n,
        compiler_params=params(8),
        cost_estimate=cost(1e6, 8 * own.size),
        name="collect",
    )(near(own), *[near(r) for r in received])


def unpack_kernel(n, where, *refs):
    core, z = where[1], where[2]
    mine, theirs, dk, dv = refs[:n], refs[n : 2 * n], refs[2 * n], refs[2 * n + 1]
    for m in range(n):
        group = jnp.bitwise_xor(z, m)
        for j, piece in enumerate((mine[m].at[0], theirs[m].at[1])):
            col = (2 * group + jnp.bitwise_xor(core, j)) * HEAD_SIZE
            col = pl.multiple_of(col, HEAD_SIZE)
            dk[:, pl.ds(col, HEAD_SIZE)] = piece[0]
            dv[:, pl.ds(col, HEAD_SIZE)] = piece[1]


def unpack(where, mine, theirs):
    n = len(mine)
    piece = mine[0].shape[2]
    out = sds((piece, KEY_VALUE_HEADS * HEAD_SIZE), jnp.bfloat16)
    return pl.pallas_call(
        functools.partial(unpack_kernel, n),
        in_specs=[SMEM] + [VMEM] * (2 * n),
        out_specs=[VMEM] * 2,
        out_shape=[out] * 2,
        compiler_params=params(8),
        cost_estimate=cost(1e6, 8 * piece * 1024),
        name="unpack_kv",
    )(where, *[near(x) for x in mine], *[near(x) for x in theirs])


def exchange(x, axis, size, m):
    return lax.ppermute(x, axis, [(i, i ^ m) for i in range(size)])


def slot_halves(n_heads):
    slots = sorted(range(n_heads), key=lambda m: (m % 2, m))
    return tuple(slots[: n_heads // 2]), tuple(slots[n_heads // 2 :])


def home_halves(n_heads):
    return tuple(range(n_heads // 2, n_heads)), tuple(range(n_heads // 2))


def local(n_chips, n_heads, queries, keys, values, outputs, out_grad, log_norm, block_order):
    where = jnp.stack([lax.axis_index("chip"), lax.axis_index("core"), lax.axis_index("head")])
    tok, cols = queries.shape
    info = jnp.concatenate([where, block_order])
    every = tuple(range(n_heads))
    halves = slot_halves(n_heads)

    zs = pack(where, keys, values, n_heads)
    zr = {0: zs[0]}
    for m in range(1, n_heads):
        zr[m] = exchange(zs[m], "head", n_heads, m)
    own_side = prepare(where, queries, out_grad, outputs, log_norm)
    q_side = list(own_side[:3]) + [exchange(x, "core", 2, 1) for x in own_side[3:]]

    other = {}
    for m in every:
        other[m] = exchange(zr[m], "core", 2, 1)
    last = n_chips - 1
    near_chips = list(range(last - 1, 0, -1))
    own, sent = [], [[] for _ in range(n_chips)]
    for a, slots in enumerate(halves):
        own.append(assemble([zr[m] for m in slots], [other[m] for m in slots]))
        for m in near_chips:
            sent[m].append(exchange(own[a], "chip", n_chips, m))
    full = halves[0] + halves[1]
    whole = assemble([zr[m] for m in full], [other[m] for m in full])
    sent[last].append(exchange(whole, "chip", n_chips, last))

    half_picks = [
        (a, j * len(slots) + i, j, slot)
        for a, slots in enumerate(halves)
        for j in range(2)
        for i, slot in enumerate(slots)
    ]
    home = home_halves(n_heads)
    home_picks = [[p for p in half_picks if p[3] in slots] for slots in home]
    far_picks = [[(0, j * n_heads + full.index(slot), j, slot) for _, _, j, slot in g] for g in home_picks]
    acc = None
    total, received, late = [], [], [[], []]
    acc, dkv = chunk(0, home_picks[:1], info, q_side, own, acc, jnp.float32)
    total.append(dkv)
    for m in near_chips:
        groups = home_picks if m == near_chips[-1] else [half_picks]
        acc, *parts = chunk(m, groups, info, q_side, sent[m], acc, jnp.bfloat16)
        for a, dkv in enumerate(parts):
            dkv = exchange(dkv, "chip", n_chips, m)
            (received if len(parts) == 1 else late[a]).append(dkv)
    for a, group in enumerate(far_picks):
        acc, dkv = chunk(last, [group], info, q_side, sent[last], acc, jnp.bfloat16)
        late[a].append(exchange(dkv, "chip", n_chips, last))
    acc, dkv = chunk(0, home_picks[1:], info, q_side, own, acc, jnp.float32)
    total.append(dkv)

    dq_own, dq_send = finish(acc, tok, cols // 2)
    dq_other = exchange(dq_send, "core", 2, 1)
    dq = place(where, dq_own, dq_other)

    back, theirs = {}, {}
    for a, slots in enumerate(home):
        wanted = [(j, slot) for j in range(2) for slot in slots]
        part = [[p[2:] for p in home_picks[a]].index(w) for w in wanted]
        full = [[p[2:] for p in half_picks].index(w) for w in wanted]
        picks = [part] + [full] * len(received) + [part] * len(late[a])
        sums = collect(picks, total[a], received + late[a])
        for slot, x in zip(slots, sums):
            back[slot] = exchange(x, "head", n_heads, slot) if slot else x
            theirs[slot] = exchange(back[slot], "core", 2, 1)
    dk, dv = unpack(where, [back[m] for m in every], [theirs[m] for m in every])
    return dq, dk, dv


def solution(mesh):
    n_seq, n_heads = mesh.shape["seq"], mesh.shape["head"]
    n_chips = n_seq // 2
    fine = Mesh(mesh.devices.reshape(n_chips, 2, n_heads), ("chip", "core", "head"))
    seq = ("chip", "core")
    rows, tokens = P(seq, "head"), P(("chip", "core", "head"), None)
    in_specs = (rows, tokens, tokens, rows, rows, P("head", seq), P())
    out_specs = (rows, tokens, tokens)

    def body(*args):
        return local(n_chips, n_heads, *args)

    return jax.shard_map(body, mesh=fine, in_specs=in_specs, out_specs=out_specs, check_vma=False)
```
